32 devices in a mesh: section: 8 (over y, x, core), tensor: 4 (over z).
Axes of the slice: x: 2, y: 2, z: 4, core: 2. Of those that a mesh axis runs over, the one named last changes fastest.
Arguments:
- section_inputs: bfloat16 [8, 512, 1024], P('section', 'tensor'), may hold values from -6 to 6
- w_in: bfloat16 [8, 2304, 1024], P('section', 'tensor'), may hold values from -0.1875 to 0.1875
- in_bias: bfloat16 [8, 2304], P('section', 'tensor'), may hold values from -3 to 3
- w_out: bfloat16 [8, 2304, 1024], P('section', 'tensor'), may hold values from -0.125 to 0.125
- out_bias: float32 [8, 1024], P('section'), may hold values from -2 to 2
- norm_gain: float32 [8, 1024], P('section'), may hold values from 0.1 to 1.9
- norm_bias: float32 [8, 1024], P('section'), may hold values from -2 to 2
- patches: bfloat16 [8, 512, 1024], P(None, 'tensor'), may hold values from -6 to 6
- plan: int32 [3], replicated, may hold values from 0 to 7, as said below
Outputs:
- received: bfloat16 [8, 4, 512, 1024], P('section', None, 'tensor')
The draws below stay inside these ranges and needn't reach their ends.
Inputs may be any that keep to these rules, and one draw needn't show every extreme that they name: `plan`: the first min(8, 3) entries are all different.
All inputs are finite; a program needn't handle non-finite values.
Results may differ from the reference program's by a relative error of at most 0.0065.
Values may be sent and summed in bfloat16 or wider, within the bound.
A program may use at most 64 MiB of HBM per device.

```python
import jax
import jax.numpy as jnp
from jax import lax

D = 1024
FF = 2304
TICKS = 4
MICRO = 8
TOKG = 512
N_SECTION = 8


def draw_plan(key, part):
    order = jax.random.permutation(key, MICRO).astype(jnp.int32)
    places = jnp.arange(TICKS - 1, dtype=jnp.int32) % MICRO
    return order[places].astype(jnp.int32)


def block_scale(key, shape, shards, least, largest):
    def one(position, parts):
        heights = jax.random.uniform(jax.random.fold_in(jax.random.fold_in(key, 6), position), (parts,), jnp.float32, least / len(shards), largest / len(shards))
        return jnp.repeat(jnp.exp(heights), shape[position] // parts).reshape((-1,) + (1,) * (len(shape) - position - 1))

    level = one(*shards[0])
    for cut in shards[1:]:
        level = level * one(*cut)
    return level


def noise(own_key, shape, scale, reach, shards=(), held_as=jnp.bfloat16):
    factor_of = block_scale(own_key, shape, shards, -0.22, 0.18) if shards else 1.0
    array = jax.random.normal(own_key, shape, jnp.float32) * scale * factor_of
    return jnp.minimum(jnp.maximum(array, -reach), reach).astype(held_as)


def setup_inputs(seed: int = 0) -> dict:
    key_of = jax.random.split(jax.random.key(seed), 10)
    section_inputs = noise(key_of[0], (N_SECTION, TOKG, D), 1.0, 6.0, ((0, 8), (1, 4)))
    w_in = noise(key_of[1], (N_SECTION, FF, D), D ** -0.5, 0.1875, ((0, 8), (1, 4)))
    in_bias = noise(key_of[2], (N_SECTION, FF), 0.5, 3.0, ((0, 8), (1, 4)))
    w_out = noise(key_of[3], (N_SECTION, FF, D), FF ** -0.5, 0.125, ((0, 8), (1, 4)))
    out_bias = noise(key_of[4], (N_SECTION, D), 0.3, 2.0, ((0, 8),), jnp.float32)
    norm_gain = jnp.clip(1.0 + 0.18 * jax.random.normal(key_of[5], (N_SECTION, D), jnp.float32), 0.1, 1.9)
    norm_bias = noise(key_of[6], (N_SECTION, D), 0.3, 2.0, ((0, 8),), jnp.float32)
    patches = noise(key_of[7], (MICRO, TOKG, D), 1.0, 6.0, ((1, 4),))
    plan = draw_plan(jax.random.fold_in(key_of[9], 71), 0)
    return {"section_inputs": section_inputs, "w_in": w_in, "in_bias": in_bias, "w_out": w_out, "out_bias": out_bias, "norm_gain": norm_gain, "norm_bias": norm_bias, "patches": patches, "plan": plan}


norm_floor = 0.1
gelu_slope = 1.702

def normalize(current, gain_row, shift_row):
    widened = current.astype(jnp.float32)
    average = lax.optimization_barrier(jnp.mean(widened, axis=-1, keepdims=True))
    centered = widened - average
    variance = lax.optimization_barrier(jnp.mean(centered * centered, axis=-1, keepdims=True))
    normed = (centered * lax.rsqrt(variance + norm_floor) * gain_row + shift_row).astype(jnp.bfloat16)
    return (normed, widened)

def activate(preact):
    return preact * jax.nn.sigmoid(gelu_slope * preact)

def apply_block(current, gain_row, shift_row, full_in, full_bias, full_out, bias_row):
    normed, widened = normalize(current, gain_row, shift_row)
    preact = lax.dot_general(normed, full_in, (((1,), (1,)), ((), ())), preferred_element_type=jnp.float32)
    preact = preact + full_bias.astype(jnp.float32)
    hidden = activate(preact).astype(jnp.bfloat16)
    return (widened + jnp.dot(hidden, full_out, preferred_element_type=jnp.float32) + bias_row).astype(jnp.bfloat16)

def reference(section_inputs, w_in, in_bias, w_out, out_bias, norm_gain, norm_bias, patches, plan):
    current = section_inputs
    records = []
    for tick_index in range(TICKS):
        produced = lax.map(lambda operands: apply_block(*operands), (current, norm_gain, norm_bias, w_in, in_bias, w_out, out_bias))
        arrived = jnp.roll(produced, 1, axis=0)
        records.append(arrived)
        if tick_index + 1 < TICKS:
            selected = lax.dynamic_index_in_dim(patches, plan[tick_index], 0, keepdims=False)
            current = arrived.at[0].set(selected)
    return jnp.stack(records, axis=1)
```

```python
import functools

import jax
import jax.numpy as jnp
from jax import lax
from jax.experimental import pallas as pl
from jax.experimental.pallas import tpu as pltpu
from jax.sharding import PartitionSpec as P

TICKS = 4
PIECES = 4
HOP_SLOTS = 2
SETTLE_LAG = 3
PASS_LAG = 2
VMEM_BYTES = 60 * 1024 * 1024

norm_floor = 0.1
gelu_slope = 1.702
MESH = pl.DeviceIdType.MESH


def activate(preact):
    return preact * jax.nn.sigmoid(gelu_slope * preact)


def normalize(widened, gain_row, shift_row):
    average = jnp.mean(widened, axis=-1, keepdims=True)
    centered = widened - average
    variance = jnp.mean(centered * centered, axis=-1, keepdims=True)
    return (centered * lax.rsqrt(variance + norm_floor) * gain_row + shift_row).astype(
        jnp.bfloat16
    )


def relay_kernel(
    n, sections, hop_slots,
    x_ref, win_hbm, ib_ref, wout_hbm, ob_ref, gain_ref, shift_ref, patches_hbm, plan_ref,
    o_ref,
    win_ref, wout_ref, patches_ref, load_sem, held, sums_in, sums_out, staged, passing, total,
    x_send, x_recv, sum_send, sum_recv, ship_send, pass_send, pass_recv, final_recv,
):
    pieces, rows = x_ref.shape[0], x_ref.shape[1]
    near, far = n // 2 - 1, n // 2
    chunks = n // 2 * pieces
    items = TICKS * chunks
    me = lax.axis_index("tensor")
    section = lax.axis_index("section")
    following = lax.rem(section + 1, sections)
    preceding = lax.rem(section + sections - 1, sections)
    carriers = [2 * tick % sections for tick in range(1, TICKS)]

    carries = section == 0
    for carrier in carriers:
        carries = carries | (section == carrier)

    loads = [
        pltpu.make_async_copy(source, target, load_sem.at[index])
        for index, (source, target) in enumerate(
            [(win_hbm, win_ref), (wout_hbm, wout_ref), (patches_hbm, patches_ref)]
        )
    ]
    for load in loads[:2]:
        load.start()
    pl.when(carries)(loads[2].start)

    def entry_side(origin):
        length = jnp.minimum(TICKS, sections - origin)
        return jnp.where(origin >= 0, lax.rem(length, 2), 0)

    def start_of(group, origin):
        return jnp.where(lax.rem(group + entry_side(origin), 2) == 0, near, far)

    my_group = jnp.where(me < n // 2, 0, 1)
    my_shard = jnp.where(me < n // 2, me, n - 1 - me)
    my_start = start_of(my_group, section)
    my_side = jnp.where(me < n // 2, near, far)

    barrier = pltpu.get_barrier_semaphore()

    def greet(sect, tensor):
        pl.semaphore_signal(
            barrier, inc=1, device_id={"section": sect, "tensor": tensor}, device_id_type=MESH
        )

    greet(following, me)
    greet(preceding, me)
    pl.when(me > 0)(lambda: greet(section, me - 1))
    pl.when(me < n - 1)(lambda: greet(section, me + 1))
    for home in range(n):
        group = home * 2 // n
        distant = jnp.abs(me - home) > 1
        pl.when(distant & (me == start_of(group, section)))(
            functools.partial(greet, section, home)
        )
        for carrier in carriers:
            if carrier and home != (near, far)[group]:
                pl.when((section == 0) & (me == (near, far)[group]))(
                    functools.partial(greet, carrier, home)
                )
    expected = 4 - jnp.where((me == 0) | (me == n - 1), 1, 0)
    expected = expected + jnp.where(jnp.abs(me - my_start) > 1, 1, 0)
    for carrier in carriers:
        if carrier:
            expected = expected + jnp.where((section == carrier) & (me != my_side), 1, 0)
    pl.semaphore_wait(barrier, expected)

    def x_copy(src, group, item, sect, tensor, send_sem):
        return pltpu.make_async_remote_copy(
            src_ref=src,
            dst_ref=held.at[group, item],
            send_sem=send_sem,
            recv_sem=x_recv.at[group, item],
            device_id={"section": sect, "tensor": tensor},
            device_id_type=MESH,
        )

    def forward_copy(way, group, item, tensor):
        return x_copy(
            held.at[group, item], group, item, section, tensor, x_send.at[way, group, item]
        )

    def relay_copy(group, item):
        return x_copy(
            sums_out.at[group, item], group, item + chunks, following, me,
            sum_send.at[group, item],
        )

    def sum_copy(way, group, item, tensor):
        return pltpu.make_async_remote_copy(
            src_ref=sums_out.at[group, item],
            dst_ref=sums_in.at[way, group, item],
            send_sem=sum_send.at[group, item],
            recv_sem=sum_recv.at[way, group, item],
            device_id={"section": section, "tensor": tensor},
            device_id_type=MESH,
        )

    def final_copy(src, send_sem, tick, piece, sect, home):
        return pltpu.make_async_remote_copy(
            src_ref=src,
            dst_ref=o_ref.at[tick, piece],
            send_sem=send_sem,
            recv_sem=final_recv.at[tick, piece],
            device_id={"section": sect, "tensor": home},
            device_id_type=MESH,
        )

    def pass_copy(group, item):
        return pltpu.make_async_remote_copy(
            src_ref=sums_out.at[group, item],
            dst_ref=passing.at[item],
            send_sem=sum_send.at[group, item],
            recv_sem=pass_recv.at[item],
            device_id={"section": following, "tensor": me},
            device_id_type=MESH,
        )

    places = (me, n - 1 - me)
    ahead = (me + 1, me - 1)
    back = (me - 1, me + 1)
    spread_lag = [
        jnp.where(at <= near, near - at, at - near) * hop_slots for at in places
    ]
    gather_lag = [
        jnp.where(at <= near, near + at, 2 * n - 2 - near - at) * hop_slots for at in places
    ]
    end_lag = (2 * n - 2 - near - far) * hop_slots

    def place(sect, side, item):
        tick, chunk = lax.div(item, chunks), lax.rem(item, chunks)
        shard, piece = lax.div(chunk, pieces), lax.rem(chunk, pieces)
        turns = jnp.minimum(tick, sect) + entry_side(sect - tick)
        group = lax.rem(turns + side, 2)
        home = jnp.where(group == 0, shard, n - 1 - shard)
        return tick, piece, home, group

    def enter(tick, piece, carry):
        item = tick * chunks + my_shard * pieces + piece
        source, start = x_ref.at[piece], my_start
        if tick:
            source, start = staged.at[tick - 1, piece], my_side
            staged[tick - 1, piece] = patches_ref[plan_ref[tick - 1], piece]
        if tick == 0:
            held[my_group, item] = source[...]
        else:

            @pl.when(section == 0)
            def _():
                held[my_group, item] = source[...]

        sends = me != start
        if tick:
            sends = sends & (section == carriers[tick - 1])

        @pl.when(sends)
        def _():
            sect = 0 if tick else section
            x_copy(source, my_group, item, sect, start, ship_send.at[tick, piece]).start()

        return carry

    lax.fori_loop(0, pieces, functools.partial(enter, 0), 0)

    @pl.when(carries)
    def _():
        loads[2].wait()
        for tick in range(1, TICKS):
            lax.fori_loop(0, pieces, functools.partial(enter, tick), 0)

    def at_slot(slot, lag):
        item = slot - lag
        return item, (item >= 0) & (item < items)

    def hands_on(side, entry, home):
        at = places[side]
        goes_back = (at > 0) & (at <= near) & jnp.logical_not(entry & (home == back[side]))
        goes_ahead = (
            (at >= near) & (at < n - 1) & jnp.logical_not(entry & (home == ahead[side]))
        )
        return goes_back, goes_ahead

    def receive(slot, side):
        item, active = at_slot(slot, spread_lag[side])

        @pl.when(active)
        def _():
            tick, piece, home, group = place(section, side, item)
            entry = (tick == 0) | (section == 0)

            @pl.when(jnp.logical_not(entry & (home == me)))
            def _():
                forward_copy(0, group, item, me).wait_recv()

            goes_back, goes_ahead = hands_on(side, entry, home)

            @pl.when(goes_ahead)
            def _():
                forward_copy(1, group, item, ahead[side]).start()

            @pl.when(goes_back)
            def _():
                forward_copy(0, group, item, back[side]).start()

            @pl.when((tick > 0) & (section > 0) & (home == me))
            def _():
                o_ref[tick - 1, piece] = held[group, item]

    def finish(slot, side):
        item, active = at_slot(slot, gather_lag[side])
        at = places[side]
        part = pl.ds(side * rows, rows)

        @pl.when(active)
        def _():
            tick, piece, home, group = place(section, side, item)

            @pl.when((at > 0) & (at <= far))
            def _():
                sum_copy(0, group, item, me).wait_recv()
                total[part] += sums_in[0, group, item].astype(jnp.float32)

            @pl.when((at >= far) & (at < n - 1))
            def _():
                sum_copy(1, group, item, me).wait_recv()
                total[part] += sums_in[1, group, item].astype(jnp.float32)

            @pl.when(at != far)
            def _():
                sums_out[group, item] = total[part].astype(jnp.bfloat16)

            @pl.when(at < far)
            def _():
                sum_copy(0, group, item, ahead[side]).start()

            @pl.when(at > far)
            def _():
                sum_copy(1, group, item, back[side]).start()

            @pl.when(at == far)
            def _():
                sums_out[group, item] = (
                    held[group, item].astype(jnp.float32) + total[part] + ob_ref[...]
                ).astype(jnp.bfloat16)
                leaves = (tick == TICKS - 1) | (following == 0)
                passes = (following == 0) & (home != me)

                @pl.when(passes)
                def _():
                    pass_copy(group, item).start()

                @pl.when(leaves & jnp.logical_not(passes))
                def _():
                    final_copy(
                        sums_out.at[group, item], sum_send.at[group, item],
                        tick, piece, following, home,
                    ).start()

                @pl.when(jnp.logical_not(leaves))
                def _():
                    relay_copy(group, item).start()

    def pass_on(slot, side, settled):
        item, active = at_slot(slot, end_lag + PASS_LAG)
        tick, piece, home, group = place(sections - 1, side, item)

        @pl.when(active & (section == 0) & (places[side] == far) & (home != me))
        def _():
            copy = final_copy(
                passing.at[item], pass_send.at[item], tick, piece, section, home
            )
            if settled:
                copy.wait_send()
            else:
                pass_copy(group, item).wait_recv()
                copy.start()

    def compute(slot):
        found = [at_slot(slot, lag) for lag in gather_lag]

        @pl.when(found[0][1] | found[1][1])
        def _():
            blocks = []
            for side in range(2):
                own, other = found[side], found[1 - side]
                group = jnp.where(
                    own[1],
                    place(section, side, own[0])[3],
                    place(section, 1 - side, other[0])[3],
                )
                blocks.append(held[group, jnp.where(own[1], own[0], other[0])])
            normed = normalize(
                jnp.concatenate(blocks, axis=0).astype(jnp.float32),
                gain_ref[...], shift_ref[...],
            )
            preact = lax.dot_general(
                normed, win_ref[...], (((1,), (1,)), ((), ())),
                preferred_element_type=jnp.float32,
            )
            hidden = activate(preact + ib_ref[...].astype(jnp.float32)).astype(jnp.bfloat16)
            total[...] = jnp.dot(hidden, wout_ref[...], preferred_element_type=jnp.float32)

        finish(slot, 0)
        finish(slot, 1)

    def settle(slot, side):
        item, active = at_slot(slot, spread_lag[side])

        @pl.when(active)
        def _():
            tick, piece, home, group = place(section, side, item)
            goes_back, goes_ahead = hands_on(side, (tick == 0) | (section == 0), home)

            @pl.when(goes_ahead)
            def _():
                forward_copy(1, group, item, me).wait_send()

            @pl.when(goes_back)
            def _():
                forward_copy(0, group, item, me).wait_send()

        summed, ready = at_slot(slot, gather_lag[side])

        @pl.when(ready)
        def _():
            group = place(section, side, summed)[3]
            sum_copy(0, group, summed, me).wait_send()

    def turn(slot, carry):
        compute(slot)
        for side in range(2):
            receive(slot + 1, side)
        for side in range(2):
            pass_on(slot, side, False)
        for side in range(2):
            settle(slot - SETTLE_LAG, side)
            pass_on(slot - SETTLE_LAG, side, True)
        return carry

    for side in range(2):
        receive(jnp.int32(0), side)
    for load in loads[:2]:
        load.wait()
    lax.fori_loop(0, items + end_lag + SETTLE_LAG + PASS_LAG, turn, 0)

    def unship(tick, piece, carry):
        start = my_side if tick else my_start
        sends = me != start
        if tick:
            sends = sends & (section == carriers[tick - 1])

        @pl.when(sends)
        def _():
            x_copy(
                staged.at[0, piece], 0, 0, section, me, ship_send.at[tick, piece]
            ).wait_send()

        return carry

    def collect(tick, piece, carry):
        final_copy(
            passing.at[0], pass_send.at[0], tick, piece, section, me
        ).wait_recv()
        return carry

    lax.fori_loop(0, pieces, functools.partial(unship, 0), 0)
    lax.fori_loop(0, pieces, functools.partial(collect, TICKS - 1), 0)

    @pl.when(carries)
    def _():
        for tick in range(1, TICKS):
            lax.fori_loop(0, pieces, functools.partial(unship, tick), 0)

    @pl.when(section == 0)
    def _():
        for tick in range(TICKS - 1):
            lax.fori_loop(0, pieces, functools.partial(collect, tick), 0)


def relay_call(n, sections, pieces, hop_slots, args):
    x, w_in, in_bias, w_out, out_bias, gain, shift, patches, plan = args
    tokens, width = x.shape
    rows = tokens // pieces
    items = TICKS * n // 2 * pieces
    micro = patches.shape[0]
    bf16 = jnp.bfloat16
    vmem = pl.BlockSpec(memory_space=pltpu.VMEM)
    hbm = pl.BlockSpec(memory_space=pl.ANY)
    every = (2, items, rows, width)
    dma = pltpu.SemaphoreType.DMA
    out = pl.pallas_call(
        functools.partial(relay_kernel, n, sections, hop_slots),
        out_shape=jax.ShapeDtypeStruct((TICKS, pieces, rows, width), bf16),
        in_specs=[vmem, hbm, vmem, hbm, vmem, vmem, vmem, hbm]
        + [pl.BlockSpec(memory_space=pltpu.SMEM)],
        out_specs=vmem,
        scratch_shapes=[
            pltpu.VMEM(w_in.shape, bf16),
            pltpu.VMEM(w_out.shape, bf16),
            pltpu.VMEM((micro, pieces, rows, width), bf16),
            dma((3,)),
            pltpu.VMEM(every, bf16),
            pltpu.VMEM((2,) + every, bf16),
            pltpu.VMEM(every, bf16),
            pltpu.VMEM((TICKS - 1, pieces, rows, width), bf16),
            pltpu.VMEM(every[1:], bf16),
            pltpu.VMEM((2 * rows, width), jnp.float32),
            dma((2, 2, items)),
            dma((2, items)),
            dma((2, items)),
            dma((2, 2, items)),
            dma((TICKS, pieces)),
            dma((items,)),
            dma((items,)),
            dma((TICKS, pieces)),
        ],
        compiler_params=pltpu.CompilerParams(
            collective_id=0, has_side_effects=True, vmem_limit_bytes=VMEM_BYTES
        ),
    )(
        x.reshape(pieces, rows, width),
        w_in,
        in_bias.reshape(1, -1),
        w_out,
        out_bias.reshape(1, -1),
        gain.reshape(1, -1),
        shift.reshape(1, -1),
        patches.reshape(micro, pieces, rows, width),
        plan,
    )
    return out.reshape(1, TICKS, tokens, width)


def passed_along(value, axis, steps):
    count = lax.axis_size(axis)
    pairs = [(source, (source + steps) % count) for source in range(count)]
    return lax.ppermute(value, axis, pairs)


def gathered_weights(args):
    current, w_in, in_bias, w_out, bias_row, gain_row, shift_row, patches, plan = args
    section_index = lax.axis_index("section")
    full_in, full_bias, full_out = (
        lax.all_gather(value, "tensor", axis=0, tiled=True) for value in (w_in, in_bias, w_out)
    )
    records = []
    for tick_index in range(TICKS):
        widened = current.astype(jnp.float32)
        normed = normalize(widened, gain_row, shift_row)
        preact = lax.dot_general(
            normed, full_in, (((1,), (1,)), ((), ())), preferred_element_type=jnp.float32
        )
        hidden = activate(preact + full_bias.astype(jnp.float32)).astype(jnp.bfloat16)
        produced = (
            widened + jnp.dot(hidden, full_out, preferred_element_type=jnp.float32) + bias_row
        ).astype(jnp.bfloat16)
        arrived = passed_along(produced, "section", 1)
        records.append(arrived)
        if tick_index + 1 < TICKS:
            selected = lax.dynamic_index_in_dim(patches, plan[tick_index], 0, keepdims=False)
            current = jnp.where(section_index == 0, selected, arrived)
    return jnp.stack(records, axis=0)[None]


def shards(n, sections, *blocks):
    args = tuple(block[0] for block in blocks[:7]) + blocks[7:]
    tokens, width = args[0].shape
    room = 2 * width * (
        tokens * (TICKS * (5 * n + 2) + 1 + args[7].shape[0]) + 2 * args[1].shape[0]
    )
    if tokens % (PIECES * 16) or n % 2 or sections < 2 or room > VMEM_BYTES * 3 // 4:
        return gathered_weights(args)
    return relay_call(n, sections, PIECES, HOP_SLOTS, args)


def solution(mesh):
    placed = (
        P("section", "tensor", None),
        P("section", "tensor", None),
        P("section", "tensor"),
        P("section", "tensor", None),
        P("section", None),
        P("section", None),
        P("section", None),
        P(None, "tensor", None),
        P(),
    )
    return jax.shard_map(
        functools.partial(shards, mesh.shape["tensor"], mesh.shape["section"]),
        mesh=mesh,
        in_specs=placed,
        out_specs=P("section", None, "tensor", None),
        check_vma=False,
    )
```

```python
import functools

import jax
import jax.numpy as jnp
from jax import lax
from jax.experimental import pallas as pl
from jax.experimental.pallas import tpu as pltpu
from jax.sharding import PartitionSpec as P

TICKS = 4
PIECES = 4
HOP_SLOTS = 2
SETTLE_LAG = 3
PASS_LAG = 2
VMEM_BYTES = 60 * 1024 * 1024

norm_floor = 0.1
gelu_slope = 1.702
MESH = pl.DeviceIdType.MESH


def activate(preact):
    return preact * jax.nn.sigmoid(gelu_slope * preact)


def normalize(widened, gain_row, shift_row):
    average = jnp.mean(widened, axis=-1, keepdims=True)
    centered = widened - average
    variance = jnp.mean(centered * centered, axis=-1, keepdims=True)
    return (centered * lax.rsqrt(variance + norm_floor) * gain_row + shift_row).astype(
        jnp.bfloat16
    )


def relay_kernel(
    n, sections, hop_slots,
    x_hbm, win_hbm, ib_hbm, wout_hbm, ob_hbm, gain_hbm, shift_hbm, patches_hbm, plan_hbm,
    o_ref,
    x_ref, win_ref, ib_ref, wout_ref, ob_ref, gain_ref, shift_ref, patches_ref, plan_ref,
    load_sem, held, sums_in, sums_out, staged, passing, total,
    x_send, x_recv, sum_send, sum_recv, ship_send, pass_send, pass_recv, final_recv,
):
    pieces, rows = x_hbm.shape[0], x_hbm.shape[1]
    near, far = n // 2 - 1, n // 2
    chunks = n // 2 * pieces
    items = TICKS * chunks
    me = lax.axis_index("tensor")
    section = lax.axis_index("section")
    following = lax.rem(section + 1, sections)
    preceding = lax.rem(section + sections - 1, sections)
    carriers = [2 * tick % sections for tick in range(1, TICKS)]

    carries = section == 0
    for carrier in carriers:
        carries = carries | (section == carrier)

    def entry_side(origin):
        length = jnp.minimum(TICKS, sections - origin)
        return jnp.where(origin >= 0, lax.rem(length, 2), 0)

    def start_of(group, origin):
        return jnp.where(lax.rem(group + entry_side(origin), 2) == 0, near, far)

    my_group = jnp.where(me < n // 2, 0, 1)
    my_shard = jnp.where(me < n // 2, me, n - 1 - me)
    my_start = start_of(my_group, section)
    my_side = jnp.where(me < n // 2, near, far)

    barrier = pltpu.get_barrier_semaphore()

    def greet(sect, tensor):
        pl.semaphore_signal(
            barrier, inc=1, device_id={"section": sect, "tensor": tensor}, device_id_type=MESH
        )

    greet(following, me)
    greet(preceding, me)
    pl.when(me > 0)(lambda: greet(section, me - 1))
    pl.when(me < n - 1)(lambda: greet(section, me + 1))
    for home in range(n):
        group = home * 2 // n
        distant = jnp.abs(me - home) > 1
        pl.when(distant & (me == start_of(group, section)))(
            functools.partial(greet, section, home)
        )
        for carrier in carriers:
            if carrier and home != (near, far)[group]:
                pl.when((section == 0) & (me == (near, far)[group]))(
                    functools.partial(greet, carrier, home)
                )
    loads = [
        pltpu.make_async_copy(source, target, load_sem.at[index])
        for index, (source, target) in enumerate(
            [
                (x_hbm, x_ref), (gain_hbm, gain_ref), (shift_hbm, shift_ref),
                (win_hbm, win_ref), (ib_hbm, ib_ref), (wout_hbm, wout_ref),
                (ob_hbm, ob_ref), (plan_hbm, plan_ref), (patches_hbm, patches_ref),
            ]
        )
    ]
    for load in loads[:7]:
        load.start()

    @pl.when(carries)
    def _():
        for load in loads[7:]:
            load.start()

    expected = 4 - jnp.where((me == 0) | (me == n - 1), 1, 0)
    expected = expected + jnp.where(jnp.abs(me - my_start) > 1, 1, 0)
    for carrier in carriers:
        if carrier:
            expected = expected + jnp.where((section == carrier) & (me != my_side), 1, 0)
    pl.semaphore_wait(barrier, expected)

    def x_copy(src, group, item, sect, tensor, send_sem):
        return pltpu.make_async_remote_copy(
            src_ref=src,
            dst_ref=held.at[group, item],
            send_sem=send_sem,
            recv_sem=x_recv.at[group, item],
            device_id={"section": sect, "tensor": tensor},
            device_id_type=MESH,
        )

    def forward_copy(way, group, item, tensor):
        return x_copy(
            held.at[group, item], group, item, section, tensor, x_send.at[way, group, item]
        )

    def relay_copy(group, item):
        return x_copy(
            sums_out.at[group, item], group, item + chunks, following, me,
            sum_send.at[group, item],
        )

    def sum_copy(way, group, item, tensor):
        return pltpu.make_async_remote_copy(
            src_ref=sums_out.at[group, item],
            dst_ref=sums_in.at[way, group, item],
            send_sem=sum_send.at[group, item],
            recv_sem=sum_recv.at[way, group, item],
            device_id={"section": section, "tensor": tensor},
            device_id_type=MESH,
        )

    def final_copy(src, send_sem, tick, piece, sect, home):
        return pltpu.make_async_remote_copy(
            src_ref=src,
            dst_ref=o_ref.at[tick, piece],
            send_sem=send_sem,
            recv_sem=final_recv.at[tick, piece],
            device_id={"section": sect, "tensor": home},
            device_id_type=MESH,
        )

    def pass_copy(group, item):
        return pltpu.make_async_remote_copy(
            src_ref=sums_out.at[group, item],
            dst_ref=passing.at[item],
            send_sem=sum_send.at[group, item],
            recv_sem=pass_recv.at[item],
            device_id={"section": following, "tensor": me},
            device_id_type=MESH,
        )

    places = (me, n - 1 - me)
    ahead = (me + 1, me - 1)
    back = (me - 1, me + 1)
    spread_lag = [
        jnp.where(at <= near, near - at, at - near) * hop_slots for at in places
    ]
    gather_lag = [
        jnp.where(at <= near, near + at, 2 * n - 2 - near - at) * hop_slots for at in places
    ]
    end_lag = (2 * n - 2 - near - far) * hop_slots

    def place(sect, side, item):
        tick, chunk = lax.div(item, chunks), lax.rem(item, chunks)
        shard, piece = lax.div(chunk, pieces), lax.rem(chunk, pieces)
        turns = jnp.minimum(tick, sect) + entry_side(sect - tick)
        group = lax.rem(turns + side, 2)
        home = jnp.where(group == 0, shard, n - 1 - shard)
        return tick, piece, home, group

    def enter(tick, piece, carry):
        item = tick * chunks + my_shard * pieces + piece
        source, start = x_ref.at[piece], my_start
        if tick:
            source, start = staged.at[tick - 1, piece], my_side
            staged[tick - 1, piece] = patches_ref[plan_ref[tick - 1], piece]
        if tick == 0:
            held[my_group, item] = source[...]
        else:

            @pl.when(section == 0)
            def _():
                held[my_group, item] = source[...]

        sends = me != start
        if tick:
            sends = sends & (section == carriers[tick - 1])

        @pl.when(sends)
        def _():
            sect = 0 if tick else section
            x_copy(source, my_group, item, sect, start, ship_send.at[tick, piece]).start()

        return carry

    loads[0].wait()
    lax.fori_loop(0, pieces, functools.partial(enter, 0), 0)

    @pl.when(carries)
    def _():
        for load in loads[7:]:
            load.wait()
        for tick in range(1, TICKS):
            lax.fori_loop(0, pieces, functools.partial(enter, tick), 0)

    def at_slot(slot, lag):
        item = slot - lag
        return item, (item >= 0) & (item < items)

    def hands_on(side, entry, home):
        at = places[side]
        goes_back = (at > 0) & (at <= near) & jnp.logical_not(entry & (home == back[side]))
        goes_ahead = (
            (at >= near) & (at < n - 1) & jnp.logical_not(entry & (home == ahead[side]))
        )
        return goes_back, goes_ahead

    def receive(slot, side):
        item, active = at_slot(slot, spread_lag[side])

        @pl.when(active)
        def _():
            tick, piece, home, group = place(section, side, item)
            entry = (tick == 0) | (section == 0)

            @pl.when(jnp.logical_not(entry & (home == me)))
            def _():
                forward_copy(0, group, item, me).wait_recv()

            goes_back, goes_ahead = hands_on(side, entry, home)

            @pl.when(goes_ahead)
            def _():
                forward_copy(1, group, item, ahead[side]).start()

            @pl.when(goes_back)
            def _():
                forward_copy(0, group, item, back[side]).start()

            @pl.when((tick > 0) & (section > 0) & (home == me))
            def _():
                o_ref[tick - 1, piece] = held[group, item]

    def finish(slot, side):
        item, active = at_slot(slot, gather_lag[side])
        at = places[side]
        part = pl.ds(side * rows, rows)

        @pl.when(active)
        def _():
            tick, piece, home, group = place(section, side, item)

            @pl.when((at > 0) & (at <= far))
            def _():
                sum_copy(0, group, item, me).wait_recv()
                total[part] += sums_in[0, group, item].astype(jnp.float32)

            @pl.when((at >= far) & (at < n - 1))
            def _():
                sum_copy(1, group, item, me).wait_recv()
                total[part] += sums_in[1, group, item].astype(jnp.float32)

            @pl.when(at != far)
            def _():
                sums_out[group, item] = total[part].astype(jnp.bfloat16)

            @pl.when(at < far)
            def _():
                sum_copy(0, group, item, ahead[side]).start()

            @pl.when(at > far)
            def _():
                sum_copy(1, group, item, back[side]).start()

            @pl.when(at == far)
            def _():
                sums_out[group, item] = (
                    held[group, item].astype(jnp.float32) + total[part] + ob_ref[...]
                ).astype(jnp.bfloat16)
                leaves = (tick == TICKS - 1) | (following == 0)
                passes = (following == 0) & (home != me) & (tick < TICKS - 1)

                @pl.when(passes)
                def _():
                    pass_copy(group, item).start()

                @pl.when(leaves & jnp.logical_not(passes))
                def _():
                    final_copy(
                        sums_out.at[group, item], sum_send.at[group, item],
                        tick, piece, following, home,
                    ).start()

                @pl.when(jnp.logical_not(leaves))
                def _():
                    relay_copy(group, item).start()

    def pass_on(slot, side, settled):
        item, active = at_slot(slot, end_lag + PASS_LAG)
        tick, piece, home, group = place(sections - 1, side, item)

        @pl.when(
            active & (section == 0) & (places[side] == far) & (home != me) & (tick < TICKS - 1)
        )
        def _():
            copy = final_copy(
                passing.at[item], pass_send.at[item], tick, piece, section, home
            )
            if settled:
                copy.wait_send()
            else:
                pass_copy(group, item).wait_recv()
                copy.start()

    def compute(slot):
        found = [at_slot(slot, lag) for lag in gather_lag]

        @pl.when(found[0][1] | found[1][1])
        def _():
            blocks = []
            for side in range(2):
                own, other = found[side], found[1 - side]
                group = jnp.where(
                    own[1],
                    place(section, side, own[0])[3],
                    place(section, 1 - side, other[0])[3],
                )
                blocks.append(held[group, jnp.where(own[1], own[0], other[0])])
            normed = normalize(
                jnp.concatenate(blocks, axis=0).astype(jnp.float32),
                gain_ref[...], shift_ref[...],
            )
            preact = lax.dot_general(
                normed, win_ref[...], (((1,), (1,)), ((), ())),
                preferred_element_type=jnp.float32,
            )
            hidden = activate(preact + ib_ref[...].astype(jnp.float32)).astype(jnp.bfloat16)
            total[...] = jnp.dot(hidden, wout_ref[...], preferred_element_type=jnp.float32)

        finish(slot, 0)
        finish(slot, 1)

    def settle(slot, side):
        item, active = at_slot(slot, spread_lag[side])

        @pl.when(active)
        def _():
            tick, piece, home, group = place(section, side, item)
            goes_back, goes_ahead = hands_on(side, (tick == 0) | (section == 0), home)

            @pl.when(goes_ahead)
            def _():
                forward_copy(1, group, item, me).wait_send()

            @pl.when(goes_back)
            def _():
                forward_copy(0, group, item, me).wait_send()

        summed, ready = at_slot(slot, gather_lag[side])

        @pl.when(ready)
        def _():
            group = place(section, side, summed)[3]
            sum_copy(0, group, summed, me).wait_send()

    def turn(slot, carry):
        compute(slot)
        for side in range(2):
            receive(slot + 1, side)
        for side in range(2):
            pass_on(slot, side, False)
        for side in range(2):
            settle(slot - SETTLE_LAG, side)
            pass_on(slot - SETTLE_LAG, side, True)
        return carry

    for side in range(2):
        receive(jnp.int32(0), side)
    for load in loads[1:7]:
        load.wait()
    lax.fori_loop(0, items + end_lag + SETTLE_LAG + PASS_LAG, turn, 0)

    def unship(tick, piece, carry):
        start = my_side if tick else my_start
        sends = me != start
        if tick:
            sends = sends & (section == carriers[tick - 1])

        @pl.when(sends)
        def _():
            x_copy(
                staged.at[0, piece], 0, 0, section, me, ship_send.at[tick, piece]
            ).wait_send()

        return carry

    def collect(tick, piece, carry):
        final_copy(
            passing.at[0], pass_send.at[0], tick, piece, section, me
        ).wait_recv()
        return carry

    lax.fori_loop(0, pieces, functools.partial(unship, 0), 0)
    lax.fori_loop(0, pieces, functools.partial(collect, TICKS - 1), 0)

    @pl.when(carries)
    def _():
        for tick in range(1, TICKS):
            lax.fori_loop(0, pieces, functools.partial(unship, tick), 0)

    @pl.when(section == 0)
    def _():
        for tick in range(TICKS - 1):
            lax.fori_loop(0, pieces, functools.partial(collect, tick), 0)


def relay_call(n, sections, pieces, hop_slots, args):
    x, w_in, in_bias, w_out, out_bias, gain, shift, patches, plan = args
    tokens, width = x.shape
    rows = tokens // pieces
    items = TICKS * n // 2 * pieces
    micro = patches.shape[0]
    bf16 = jnp.bfloat16
    vmem = pl.BlockSpec(memory_space=pltpu.VMEM)
    every = (2, items, rows, width)
    dma = pltpu.SemaphoreType.DMA
    out = pl.pallas_call(
        functools.partial(relay_kernel, n, sections, hop_slots),
        out_shape=pltpu.VMEM((TICKS, pieces, rows, width), bf16),
        in_specs=[pl.BlockSpec(memory_space=pl.ANY)] * 9,
        out_specs=vmem,
        scratch_shapes=[
            pltpu.VMEM((pieces, rows, width), bf16),
            pltpu.VMEM(w_in.shape, bf16),
            pltpu.VMEM((1, w_in.shape[0]), bf16),
            pltpu.VMEM(w_out.shape, bf16),
            pltpu.VMEM((1, width), jnp.float32),
            pltpu.VMEM((1, width), jnp.float32),
            pltpu.VMEM((1, width), jnp.float32),
            pltpu.VMEM((micro, pieces, rows, width), bf16),
            pltpu.SMEM(plan.shape, jnp.int32),
            dma((9,)),
            pltpu.VMEM(every, bf16),
            pltpu.VMEM((2,) + every, bf16),
            pltpu.VMEM(every, bf16),
            pltpu.VMEM((TICKS - 1, pieces, rows, width), bf16),
            pltpu.VMEM(every[1:], bf16),
            pltpu.VMEM((2 * rows, width), jnp.float32),
            dma((2, 2, items)),
            dma((2, items)),
            dma((2, items)),
            dma((2, 2, items)),
            dma((TICKS, pieces)),
            dma((items,)),
            dma((items,)),
            dma((TICKS, pieces)),
        ],
        compiler_params=pltpu.CompilerParams(
            collective_id=0, has_side_effects=True, vmem_limit_bytes=VMEM_BYTES
        ),
    )(
        x.reshape(pieces, rows, width),
        w_in,
        in_bias.reshape(1, -1),
        w_out,
        out_bias.reshape(1, -1),
        gain.reshape(1, -1),
        shift.reshape(1, -1),
        patches.reshape(micro, pieces, rows, width),
        plan,
    )
    return out.reshape(1, TICKS, tokens, width)


def passed_along(value, axis, steps):
    count = lax.axis_size(axis)
    pairs = [(source, (source + steps) % count) for source in range(count)]
    return lax.ppermute(value, axis, pairs)


def gathered_weights(args):
    current, w_in, in_bias, w_out, bias_row, gain_row, shift_row, patches, plan = args
    section_index = lax.axis_index("section")
    full_in, full_bias, full_out = (
        lax.all_gather(value, "tensor", axis=0, tiled=True) for value in (w_in, in_bias, w_out)
    )
    records = []
    for tick_index in range(TICKS):
        widened = current.astype(jnp.float32)
        normed = normalize(widened, gain_row, shift_row)
        preact = lax.dot_general(
            normed, full_in, (((1,), (1,)), ((), ())), preferred_element_type=jnp.float32
        )
        hidden = activate(preact + full_bias.astype(jnp.float32)).astype(jnp.bfloat16)
        produced = (
            widened + jnp.dot(hidden, full_out, preferred_element_type=jnp.float32) + bias_row
        ).astype(jnp.bfloat16)
        arrived = passed_along(produced, "section", 1)
        records.append(arrived)
        if tick_index + 1 < TICKS:
            selected = lax.dynamic_index_in_dim(patches, plan[tick_index], 0, keepdims=False)
            current = jnp.where(section_index == 0, selected, arrived)
    return jnp.stack(records, axis=0)[None]


def shards(n, sections, *blocks):
    args = tuple(block[0] for block in blocks[:7]) + blocks[7:]
    tokens, width = args[0].shape
    room = 2 * width * (
        tokens * (TICKS * (5 * n + 2) + 1 + args[7].shape[0]) + 2 * args[1].shape[0]
    )
    if tokens % (PIECES * 16) or n % 2 or sections < 2 or room > VMEM_BYTES * 3 // 4:
        return gathered_weights(args)
    return relay_call(n, sections, PIECES, HOP_SLOTS, args)


def solution(mesh):
    placed = (
        P("section", "tensor", None),
        P("section", "tensor", None),
        P("section", "tensor"),
        P("section", "tensor", None),
        P("section", None),
        P("section", None),
        P("section", None),
        P(None, "tensor", None),
        P(),
    )
    return jax.shard_map(
        functools.partial(shards, mesh.shape["tensor"], mesh.shape["section"]),
        mesh=mesh,
        in_specs=placed,
        out_specs=P("section", None, "tensor", None),
        check_vma=False,
    )
```

```python
import functools

import jax
import jax.numpy as jnp
from jax import lax
from jax.experimental import pallas as pl
from jax.experimental.pallas import tpu as pltpu
from jax.sharding import PartitionSpec as P

TICKS = 4
PIECES = 4
HOP_SLOTS = 2
SETTLE_LAG = 3
SEND_RING = 4
PASS_LAG = 2
VMEM_BYTES = 60 * 1024 * 1024

norm_floor = 0.1
gelu_slope = 1.702
MESH = pl.DeviceIdType.MESH


def activate(preact):
    return preact * jax.nn.sigmoid(gelu_slope * preact)


def normalize(widened, gain_row, shift_row):
    average = jnp.mean(widened, axis=-1, keepdims=True)
    centered = widened - average
    variance = jnp.mean(centered * centered, axis=-1, keepdims=True)
    return (centered * lax.rsqrt(variance + norm_floor) * gain_row + shift_row).astype(
        jnp.bfloat16
    )


def relay_kernel(
    n, sections, hop_slots,
    x_hbm, win_hbm, ib_hbm, wout_hbm, ob_hbm, gain_hbm, shift_hbm, patches_hbm, plan_hbm,
    o_ref,
    x_ref, win_ref, ib_ref, wout_ref, ob_ref, gain_ref, shift_ref, patches_ref, plan_ref,
    load_sem, held, sums_in, sums_out, staged, passing, total,
    x_send, x_recv, relay_recv, sum_send, sum_recv, ship_send, pass_send, pass_recv, final_recv,
):
    pieces, rows = x_hbm.shape[0], x_hbm.shape[1]
    near, far = n // 2 - 1, n // 2
    chunks = n // 2 * pieces
    items = TICKS * chunks
    me = lax.axis_index("tensor")
    section = lax.axis_index("section")
    following = lax.rem(section + 1, sections)
    preceding = lax.rem(section + sections - 1, sections)
    carriers = [2 * tick % sections for tick in range(1, TICKS)]

    carries = section == 0
    for carrier in carriers:
        carries = carries | (section == carrier)

    def entry_side(origin):
        length = jnp.minimum(TICKS, sections - origin)
        return jnp.where(origin >= 0, lax.rem(length, 2), 0)

    def start_of(group, origin):
        return jnp.where(lax.rem(group + entry_side(origin), 2) == 0, near, far)

    my_group = jnp.where(me < n // 2, 0, 1)
    my_shard = jnp.where(me < n // 2, me, n - 1 - me)
    my_start = start_of(my_group, section)
    my_side = jnp.where(me < n // 2, near, far)

    barrier = pltpu.get_barrier_semaphore()

    def greet(sect, tensor):
        pl.semaphore_signal(
            barrier, inc=1, device_id={"section": sect, "tensor": tensor}, device_id_type=MESH
        )

    greet(following, me)
    greet(preceding, me)
    pl.when(me > 0)(lambda: greet(section, me - 1))
    pl.when(me < n - 1)(lambda: greet(section, me + 1))
    for home in range(n):
        group = home * 2 // n
        distant = jnp.abs(me - home) > 1
        pl.when(distant & (me == start_of(group, section)))(
            functools.partial(greet, section, home)
        )
        for carrier in carriers:
            if carrier and home != (near, far)[group]:
                pl.when((section == 0) & (me == (near, far)[group]))(
                    functools.partial(greet, carrier, home)
                )
    loads = [
        pltpu.make_async_copy(source, target, load_sem.at[index])
        for index, (source, target) in enumerate(
            [
                (x_hbm, x_ref), (gain_hbm, gain_ref), (shift_hbm, shift_ref),
                (win_hbm, win_ref), (ib_hbm, ib_ref), (wout_hbm, wout_ref),
                (ob_hbm, ob_ref), (plan_hbm, plan_ref), (patches_hbm, patches_ref),
            ]
        )
    ]
    for load in loads[:7]:
        load.start()

    @pl.when(carries)
    def _():
        for load in loads[7:]:
            load.start()

    expected = 4 - jnp.where((me == 0) | (me == n - 1), 1, 0)
    expected = expected + jnp.where(jnp.abs(me - my_start) > 1, 1, 0)
    for carrier in carriers:
        if carrier:
            expected = expected + jnp.where((section == carrier) & (me != my_side), 1, 0)
    pl.semaphore_wait(barrier, expected)

    def x_copy(src, group, item, sect, tensor, send_sem, recv_sem):
        return pltpu.make_async_remote_copy(
            src_ref=src,
            dst_ref=held.at[group, item],
            send_sem=send_sem,
            recv_sem=recv_sem,
            device_id={"section": sect, "tensor": tensor},
            device_id_type=MESH,
        )

    def spread_sem(group, item):
        return x_recv.at[group, lax.rem(item, chunks)]

    def forward_copy(way, side, group, item, tensor):
        return x_copy(
            held.at[group, item], group, item, section, tensor,
            x_send.at[way, side, lax.rem(item, SEND_RING)], spread_sem(group, item),
        )

    def outgoing(side, item):
        return sum_send.at[side, lax.rem(item, SEND_RING)]

    def relay_copy(side, group, item):
        return x_copy(
            sums_out.at[group, item], group, item + chunks, following, me,
            outgoing(side, item), relay_recv.at[item],
        )

    def sum_copy(way, side, group, item, tensor):
        return pltpu.make_async_remote_copy(
            src_ref=sums_out.at[group, item],
            dst_ref=sums_in.at[way, group, item],
            send_sem=outgoing(side, item),
            recv_sem=sum_recv.at[way, group, lax.rem(item, chunks)],
            device_id={"section": section, "tensor": tensor},
            device_id_type=MESH,
        )

    def final_copy(src, send_sem, tick, piece, sect, home):
        return pltpu.make_async_remote_copy(
            src_ref=src,
            dst_ref=o_ref.at[tick, piece],
            send_sem=send_sem,
            recv_sem=final_recv.at[tick, piece],
            device_id={"section": sect, "tensor": home},
            device_id_type=MESH,
        )

    def pass_copy(side, group, item, tick, piece):
        return pltpu.make_async_remote_copy(
            src_ref=sums_out.at[group, item],
            dst_ref=passing.at[tick, piece],
            send_sem=outgoing(side, item),
            recv_sem=pass_recv.at[tick, piece],
            device_id={"section": following, "tensor": me},
            device_id_type=MESH,
        )

    places = (me, n - 1 - me)
    ahead = (me + 1, me - 1)
    back = (me - 1, me + 1)
    spread_lag = [
        jnp.where(at <= near, near - at, at - near) * hop_slots for at in places
    ]
    gather_lag = [
        jnp.where(at <= near, near + at, 2 * n - 2 - near - at) * hop_slots for at in places
    ]
    end_lag = (2 * n - 2 - near - far) * hop_slots

    def place(sect, side, item):
        tick, chunk = lax.div(item, chunks), lax.rem(item, chunks)
        shard, piece = lax.div(chunk, pieces), lax.rem(chunk, pieces)
        turns = jnp.minimum(tick, sect) + entry_side(sect - tick)
        group = lax.rem(turns + side, 2)
        home = jnp.where(group == 0, shard, n - 1 - shard)
        return tick, piece, home, group

    def enter(tick, piece, carry):
        item = tick * chunks + my_shard * pieces + piece
        source, start = x_ref.at[piece], my_start
        if tick:
            source, start = staged.at[tick - 1, piece], my_side
            staged[tick - 1, piece] = patches_ref[plan_ref[tick - 1], piece]
        if tick == 0:
            held[my_group, item] = source[...]
        else:

            @pl.when(section == 0)
            def _():
                held[my_group, item] = source[...]

        sends = me != start
        if tick:
            sends = sends & (section == carriers[tick - 1])

        @pl.when(sends)
        def _():
            sect = 0 if tick else section
            arrival = relay_recv.at[item - chunks] if tick else spread_sem(my_group, item)
            x_copy(
                source, my_group, item, sect, start, ship_send.at[tick, piece], arrival
            ).start()

        return carry

    loads[0].wait()
    lax.fori_loop(0, pieces, functools.partial(enter, 0), 0)

    @pl.when(carries)
    def _():
        for load in loads[7:]:
            load.wait()
        for tick in range(1, TICKS):
            lax.fori_loop(0, pieces, functools.partial(enter, tick), 0)

    def at_slot(slot, lag):
        item = slot - lag
        return item, (item >= 0) & (item < items)

    def hands_on(side, entry, home):
        at = places[side]
        goes_back = (at > 0) & (at <= near) & jnp.logical_not(entry & (home == back[side]))
        goes_ahead = (
            (at >= near) & (at < n - 1) & jnp.logical_not(entry & (home == ahead[side]))
        )
        return goes_back, goes_ahead

    def receive(slot, side):
        item, active = at_slot(slot, spread_lag[side])

        @pl.when(active)
        def _():
            tick, piece, home, group = place(section, side, item)
            entry = (tick == 0) | (section == 0)

            arrives = jnp.logical_not(entry & (home == me))
            starts = (places[side] == near) & (tick > 0)

            @pl.when(arrives & starts)
            def _():
                relay_copy(side, group, item - chunks).wait_recv()

            @pl.when(arrives & jnp.logical_not(starts))
            def _():
                forward_copy(0, side, group, item, me).wait_recv()

            goes_back, goes_ahead = hands_on(side, entry, home)

            @pl.when(goes_ahead)
            def _():
                forward_copy(1, side, group, item, ahead[side]).start()

            @pl.when(goes_back)
            def _():
                forward_copy(0, side, group, item, back[side]).start()

            @pl.when((tick > 0) & (section > 0) & (home == me))
            def _():
                o_ref[tick - 1, piece] = held[group, item]

    def finish(slot, side):
        item, active = at_slot(slot, gather_lag[side])
        at = places[side]
        part = pl.ds(side * rows, rows)

        @pl.when(active)
        def _():
            tick, piece, home, group = place(section, side, item)

            @pl.when((at > 0) & (at <= far))
            def _():
                sum_copy(0, side, group, item, me).wait_recv()
                total[part] += sums_in[0, group, item].astype(jnp.float32)

            @pl.when((at >= far) & (at < n - 1))
            def _():
                sum_copy(1, side, group, item, me).wait_recv()
                total[part] += sums_in[1, group, item].astype(jnp.float32)

            @pl.when(at != far)
            def _():
                sums_out[group, item] = total[part].astype(jnp.bfloat16)

            @pl.when(at < far)
            def _():
                sum_copy(0, side, group, item, ahead[side]).start()

            @pl.when(at > far)
            def _():
                sum_copy(1, side, group, item, back[side]).start()

            @pl.when(at == far)
            def _():
                sums_out[group, item] = (
                    held[group, item].astype(jnp.float32) + total[part] + ob_ref[...]
                ).astype(jnp.bfloat16)
                leaves = (tick == TICKS - 1) | (following == 0)
                passes = (following == 0) & (home != me) & (tick < TICKS - 1)

                @pl.when(passes)
                def _():
                    pass_copy(side, group, item, tick, piece).start()

                @pl.when(leaves & jnp.logical_not(passes))
                def _():
                    final_copy(
                        sums_out.at[group, item], outgoing(side, item),
                        tick, piece, following, home,
                    ).start()

                @pl.when(jnp.logical_not(leaves))
                def _():
                    relay_copy(side, group, item).start()

    def pass_on(slot, side, settled):
        item, active = at_slot(slot, end_lag + PASS_LAG)
        tick, piece, home, group = place(sections - 1, side, item)

        @pl.when(
            active & (section == 0) & (places[side] == far) & (home != me) & (tick < TICKS - 1)
        )
        def _():
            copy = final_copy(
                passing.at[tick, piece], pass_send.at[piece], tick, piece, section, home
            )
            if settled:
                copy.wait_send()
            else:
                pass_copy(side, group, item, tick, piece).wait_recv()
                copy.start()

    def compute(slot):
        found = [at_slot(slot, lag) for lag in gather_lag]

        @pl.when(found[0][1] | found[1][1])
        def _():
            blocks = []
            for side in range(2):
                own, other = found[side], found[1 - side]
                group = jnp.where(
                    own[1],
                    place(section, side, own[0])[3],
                    place(section, 1 - side, other[0])[3],
                )
                blocks.append(held[group, jnp.where(own[1], own[0], other[0])])
            normed = normalize(
                jnp.concatenate(blocks, axis=0).astype(jnp.float32),
                gain_ref[...], shift_ref[...],
            )
            preact = lax.dot_general(
                normed, win_ref[...], (((1,), (1,)), ((), ())),
                preferred_element_type=jnp.float32,
            )
            hidden = activate(preact + ib_ref[...].astype(jnp.float32)).astype(jnp.bfloat16)
            total[...] = jnp.dot(hidden, wout_ref[...], preferred_element_type=jnp.float32)

        finish(slot, 0)
        finish(slot, 1)

    def settle(slot, side):
        item, active = at_slot(slot, spread_lag[side])

        @pl.when(active)
        def _():
            tick, piece, home, group = place(section, side, item)
            goes_back, goes_ahead = hands_on(side, (tick == 0) | (section == 0), home)

            @pl.when(goes_ahead)
            def _():
                forward_copy(1, side, group, item, me).wait_send()

            @pl.when(goes_back)
            def _():
                forward_copy(0, side, group, item, me).wait_send()

        summed, ready = at_slot(slot, gather_lag[side])

        @pl.when(ready)
        def _():
            sum_copy(0, side, 0, summed, me).wait_send()

    def turn(slot, carry):
        compute(slot)
        for side in range(2):
            settle(slot - SETTLE_LAG, side)
            receive(slot + 1, side)
        for side in range(2):
            pass_on(slot - SETTLE_LAG, side, True)
            pass_on(slot, side, False)
        return carry

    for side in range(2):
        receive(jnp.int32(0), side)
    for load in loads[1:7]:
        load.wait()
    lax.fori_loop(0, items + end_lag + SETTLE_LAG + PASS_LAG, turn, 0)

    def unship(tick, piece, carry):
        start = my_side if tick else my_start
        sends = me != start
        if tick:
            sends = sends & (section == carriers[tick - 1])

        @pl.when(sends)
        def _():
            x_copy(
                staged.at[0, piece], 0, 0, section, me, ship_send.at[tick, piece],
                spread_sem(0, 0),
            ).wait_send()

        return carry

    def collect(tick, piece, carry):
        final_copy(
            passing.at[0, 0], pass_send.at[0], tick, piece, section, me
        ).wait_recv()
        return carry

    lax.fori_loop(0, pieces, functools.partial(unship, 0), 0)
    lax.fori_loop(0, pieces, functools.partial(collect, TICKS - 1), 0)

    @pl.when(carries)
    def _():
        for tick in range(1, TICKS):
            lax.fori_loop(0, pieces, functools.partial(unship, tick), 0)

    @pl.when(section == 0)
    def _():
        for tick in range(TICKS - 1):
            lax.fori_loop(0, pieces, functools.partial(collect, tick), 0)


def relay_call(n, sections, pieces, hop_slots, args):
    x, w_in, in_bias, w_out, out_bias, gain, shift, patches, plan = args
    tokens, width = x.shape
    rows = tokens // pieces
    chunks = n // 2 * pieces
    items = TICKS * chunks
    micro = patches.shape[0]
    bf16 = jnp.bfloat16
    vmem = pl.BlockSpec(memory_space=pltpu.VMEM)
    every = (2, items, rows, width)
    dma = pltpu.SemaphoreType.DMA
    out = pl.pallas_call(
        functools.partial(relay_kernel, n, sections, hop_slots),
        out_shape=pltpu.VMEM((TICKS, pieces, rows, width), bf16),
        in_specs=[pl.BlockSpec(memory_space=pl.ANY)] * 9,
        out_specs=vmem,
        scratch_shapes=[
            pltpu.VMEM((pieces, rows, width), bf16),
            pltpu.VMEM(w_in.shape, bf16),
            pltpu.VMEM((1, w_in.shape[0]), bf16),
            pltpu.VMEM(w_out.shape, bf16),
            pltpu.VMEM((1, width), jnp.float32),
            pltpu.VMEM((1, width), jnp.float32),
            pltpu.VMEM((1, width), jnp.float32),
            pltpu.VMEM((micro, pieces, rows, width), bf16),
            pltpu.SMEM(plan.shape, jnp.int32),
            dma((9,)),
            pltpu.VMEM(every, bf16),
            pltpu.VMEM((2,) + every, bf16),
            pltpu.VMEM(every, bf16),
            pltpu.VMEM((TICKS - 1, pieces, rows, width), bf16),
            pltpu.VMEM((TICKS - 1, pieces, rows, width), bf16),
            pltpu.VMEM((2 * rows, width), jnp.float32),
            dma((2, 2, SEND_RING)),
            dma((2, chunks)),
            dma((items - chunks,)),
            dma((2, SEND_RING)),
            dma((2, 2, chunks)),
            dma((TICKS, pieces)),
            dma((pieces,)),
            dma((TICKS - 1, pieces)),
            dma((TICKS, pieces)),
        ],
        compiler_params=pltpu.CompilerParams(
            collective_id=0, has_side_effects=True, vmem_limit_bytes=VMEM_BYTES
        ),
    )(
        x.reshape(pieces, rows, width),
        w_in,
        in_bias.reshape(1, -1),
        w_out,
        out_bias.reshape(1, -1),
        gain.reshape(1, -1),
        shift.reshape(1, -1),
        patches.reshape(micro, pieces, rows, width),
        plan,
    )
    return out.reshape(1, TICKS, tokens, width)


def passed_along(value, axis, steps):
    count = lax.axis_size(axis)
    pairs = [(source, (source + steps) % count) for source in range(count)]
    return lax.ppermute(value, axis, pairs)


def gathered_weights(args):
    current, w_in, in_bias, w_out, bias_row, gain_row, shift_row, patches, plan = args
    section_index = lax.axis_index("section")
    full_in, full_bias, full_out = (
        lax.all_gather(value, "tensor", axis=0, tiled=True) for value in (w_in, in_bias, w_out)
    )
    records = []
    for tick_index in range(TICKS):
        widened = current.astype(jnp.float32)
        normed = normalize(widened, gain_row, shift_row)
        preact = lax.dot_general(
            normed, full_in, (((1,), (1,)), ((), ())), preferred_element_type=jnp.float32
        )
        hidden = activate(preact + full_bias.astype(jnp.float32)).astype(jnp.bfloat16)
        produced = (
            widened + jnp.dot(hidden, full_out, preferred_element_type=jnp.float32) + bias_row
        ).astype(jnp.bfloat16)
        arrived = passed_along(produced, "section", 1)
        records.append(arrived)
        if tick_index + 1 < TICKS:
            selected = lax.dynamic_index_in_dim(patches, plan[tick_index], 0, keepdims=False)
            current = jnp.where(section_index == 0, selected, arrived)
    return jnp.stack(records, axis=0)[None]


def shards(n, sections, *blocks):
    args = tuple(block[0] for block in blocks[:7]) + blocks[7:]
    tokens, width = args[0].shape
    room = 2 * width * (
        tokens * (TICKS * (5 * n + 2) + 1 + args[7].shape[0]) + 2 * args[1].shape[0]
    )
    if tokens % (PIECES * 16) or n % 2 or sections < 2 or room > VMEM_BYTES * 3 // 4:
        return gathered_weights(args)
    return relay_call(n, sections, PIECES, HOP_SLOTS, args)


def solution(mesh):
    placed = (
        P("section", "tensor", None),
        P("section", "tensor", None),
        P("section", "tensor"),
        P("section", "tensor", None),
        P("section", None),
        P("section", None),
        P("section", None),
        P(None, "tensor", None),
        P(),
    )
    return jax.shard_map(
        functools.partial(shards, mesh.shape["tensor"], mesh.shape["section"]),
        mesh=mesh,
        in_specs=placed,
        out_specs=P("section", None, "tensor", None),
        check_vma=False,
    )
```

```python
import functools

import jax
import jax.numpy as jnp
from jax import lax
from jax.experimental import pallas as pl
from jax.experimental.pallas import tpu as pltpu
from jax.sharding import PartitionSpec as P

TICKS = 4
PIECES = 4
HOP_SLOTS = 2
SETTLE_LAG = 3
SEND_RING = 4
PASS_LAG = 2
VMEM_BYTES = 60 * 1024 * 1024

norm_floor = 0.1
gelu_slope = 1.702
MESH = pl.DeviceIdType.MESH


def activate(preact):
    return preact * jax.nn.sigmoid(gelu_slope * preact)


def normalize(widened, gain_row, shift_row):
    average = jnp.mean(widened, axis=-1, keepdims=True)
    centered = widened - average
    variance = jnp.mean(centered * centered, axis=-1, keepdims=True)
    return (centered * lax.rsqrt(variance + norm_floor) * gain_row + shift_row).astype(
        jnp.bfloat16
    )


def relay_kernel(
    n, sections, hop_slots,
    x_hbm, win_hbm, ib_hbm, wout_hbm, ob_hbm, gain_hbm, shift_hbm, patches_hbm, plan_hbm,
    o_ref,
    x_ref, win_ref, ib_ref, wout_ref, ob_ref, gain_ref, shift_ref, patches_ref, plan_ref,
    load_sem, held, sums_in, sums_out, staged, passing, total,
    x_send, x_recv, relay_recv, sum_send, sum_recv, ship_send, pass_send, pass_recv, final_recv,
):
    pieces, rows = x_hbm.shape[0], x_hbm.shape[1]
    near, far = n // 2 - 1, n // 2
    chunks = n // 2 * pieces
    items = TICKS * chunks
    me = lax.axis_index("tensor")
    section = lax.axis_index("section")
    following = lax.rem(section + 1, sections)
    preceding = lax.rem(section + sections - 1, sections)
    carriers = [2 * tick % sections for tick in range(1, TICKS)]

    carries = section == 0
    for carrier in carriers:
        carries = carries | (section == carrier)

    def entry_side(origin):
        length = jnp.minimum(TICKS, sections - origin)
        return jnp.where(origin >= 0, lax.rem(length, 2), 0)

    def start_of(group, origin):
        return jnp.where(lax.rem(group + entry_side(origin), 2) == 0, near, far)

    my_group = jnp.where(me < n // 2, 0, 1)
    my_shard = jnp.where(me < n // 2, me, n - 1 - me)
    my_start = start_of(my_group, section)
    my_side = jnp.where(me < n // 2, near, far)

    barrier = pltpu.get_barrier_semaphore()

    def greet(sect, tensor):
        pl.semaphore_signal(
            barrier, inc=1, device_id={"section": sect, "tensor": tensor}, device_id_type=MESH
        )

    greet(following, me)
    greet(preceding, me)
    pl.when(me > 0)(lambda: greet(section, me - 1))
    pl.when(me < n - 1)(lambda: greet(section, me + 1))
    for home in range(n):
        group = home * 2 // n
        distant = jnp.abs(me - home) > 1
        pl.when(distant & (me == start_of(group, section)))(
            functools.partial(greet, section, home)
        )
        for carrier in carriers:
            if carrier and home != (near, far)[group]:
                pl.when((section == 0) & (me == (near, far)[group]))(
                    functools.partial(greet, carrier, home)
                )
    loads = [
        pltpu.make_async_copy(source, target, load_sem.at[index])
        for index, (source, target) in enumerate(
            [
                (x_hbm, x_ref), (gain_hbm, gain_ref), (shift_hbm, shift_ref),
                (win_hbm, win_ref), (ib_hbm, ib_ref), (wout_hbm, wout_ref),
                (ob_hbm, ob_ref), (plan_hbm, plan_ref), (patches_hbm, patches_ref),
            ]
        )
    ]
    for load in loads[:7]:
        load.start()

    @pl.when(carries)
    def _():
        for load in loads[7:]:
            load.start()

    expected = 4 - jnp.where((me == 0) | (me == n - 1), 1, 0)
    expected = expected + jnp.where(jnp.abs(me - my_start) > 1, 1, 0)
    for carrier in carriers:
        if carrier:
            expected = expected + jnp.where((section == carrier) & (me != my_side), 1, 0)
    pl.semaphore_wait(barrier, expected)

    def x_copy(src, group, item, sect, tensor, send_sem, recv_sem):
        return pltpu.make_async_remote_copy(
            src_ref=src,
            dst_ref=held.at[group, item],
            send_sem=send_sem,
            recv_sem=recv_sem,
            device_id={"section": sect, "tensor": tensor},
            device_id_type=MESH,
        )

    def spread_sem(group, item):
        return x_recv.at[group, lax.rem(item, chunks)]

    def forward_copy(way, side, group, item, tensor):
        return x_copy(
            held.at[group, item], group, item, section, tensor,
            x_send.at[way, side, lax.rem(item, SEND_RING)], spread_sem(group, item),
        )

    def outgoing(side, item):
        return sum_send.at[side, lax.rem(item, SEND_RING)]

    def relay_copy(side, group, item):
        return x_copy(
            sums_out.at[group, item], group, item + chunks, following, me,
            outgoing(side, item), relay_recv.at[item],
        )

    def sum_copy(way, side, group, item, tensor):
        return pltpu.make_async_remote_copy(
            src_ref=sums_out.at[group, item],
            dst_ref=sums_in.at[way, group, item],
            send_sem=outgoing(side, item),
            recv_sem=sum_recv.at[way, group, lax.rem(item, chunks)],
            device_id={"section": section, "tensor": tensor},
            device_id_type=MESH,
        )

    def final_copy(src, send_sem, tick, piece, sect, home):
        return pltpu.make_async_remote_copy(
            src_ref=src,
            dst_ref=o_ref.at[tick, piece],
            send_sem=send_sem,
            recv_sem=final_recv.at[tick],
            device_id={"section": sect, "tensor": home},
            device_id_type=MESH,
        )

    def pass_copy(side, group, item, tick, piece):
        return pltpu.make_async_remote_copy(
            src_ref=sums_out.at[group, item],
            dst_ref=passing.at[tick, piece],
            send_sem=outgoing(side, item),
            recv_sem=pass_recv.at[tick, piece],
            device_id={"section": following, "tensor": me},
            device_id_type=MESH,
        )

    places = (me, n - 1 - me)
    ahead = (me + 1, me - 1)
    back = (me - 1, me + 1)
    spread_lag = [
        jnp.where(at <= near, near - at, at - near) * hop_slots for at in places
    ]
    gather_lag = [
        jnp.where(at <= near, near + at, 2 * n - 2 - near - at) * hop_slots for at in places
    ]
    end_lag = (2 * n - 2 - near - far) * hop_slots

    def place(sect, side, item):
        tick, chunk = lax.div(item, chunks), lax.rem(item, chunks)
        shard, piece = lax.div(chunk, pieces), lax.rem(chunk, pieces)
        turns = jnp.minimum(tick, sect) + entry_side(sect - tick)
        group = lax.rem(turns + side, 2)
        home = jnp.where(group == 0, shard, n - 1 - shard)
        return tick, piece, home, group

    def enter(tick, piece, carry):
        item = tick * chunks + my_shard * pieces + piece
        source, start = x_ref.at[piece], my_start
        if tick:
            source, start = staged.at[tick - 1, piece], my_side
            staged[tick - 1, piece] = patches_ref[plan_ref[tick - 1], piece]
        if tick == 0:
            held[my_group, item] = source[...]
        else:

            @pl.when(section == 0)
            def _():
                held[my_group, item] = source[...]

        sends = me != start
        if tick:
            sends = sends & (section == carriers[tick - 1])

        @pl.when(sends)
        def _():
            sect = 0 if tick else section
            arrival = relay_recv.at[item - chunks] if tick else spread_sem(my_group, item)
            x_copy(
                source, my_group, item, sect, start, ship_send.at[tick], arrival
            ).start()

        return carry

    loads[0].wait()
    lax.fori_loop(0, pieces, functools.partial(enter, 0), 0)

    @pl.when(carries)
    def _():
        for load in loads[7:]:
            load.wait()
        for tick in range(1, TICKS):
            lax.fori_loop(0, pieces, functools.partial(enter, tick), 0)

    def at_slot(slot, lag):
        item = slot - lag
        return item, (item >= 0) & (item < items)

    def hands_on(side, entry, home):
        at = places[side]
        goes_back = (at > 0) & (at <= near) & jnp.logical_not(entry & (home == back[side]))
        goes_ahead = (
            (at >= near) & (at < n - 1) & jnp.logical_not(entry & (home == ahead[side]))
        )
        return goes_back, goes_ahead

    def receive(slot, side):
        item, active = at_slot(slot, spread_lag[side])

        @pl.when(active)
        def _():
            tick, piece, home, group = place(section, side, item)
            entry = (tick == 0) | (section == 0)

            arrives = jnp.logical_not(entry & (home == me))
            starts = (places[side] == near) & (tick > 0)

            @pl.when(arrives & starts)
            def _():
                relay_copy(side, group, item - chunks).wait_recv()

            @pl.when(arrives & jnp.logical_not(starts))
            def _():
                forward_copy(0, side, group, item, me).wait_recv()

            goes_back, goes_ahead = hands_on(side, entry, home)

            @pl.when(goes_ahead)
            def _():
                forward_copy(1, side, group, item, ahead[side]).start()

            @pl.when(goes_back)
            def _():
                forward_copy(0, side, group, item, back[side]).start()

            @pl.when((tick > 0) & (section > 0) & (home == me))
            def _():
                o_ref[tick - 1, piece] = held[group, item]

    def finish(slot, side):
        item, active = at_slot(slot, gather_lag[side])
        at = places[side]
        part = pl.ds(side * rows, rows)

        @pl.when(active)
        def _():
            tick, piece, home, group = place(section, side, item)

            @pl.when((at > 0) & (at <= far))
            def _():
                sum_copy(0, side, group, item, me).wait_recv()
                total[part] += sums_in[0, group, item].astype(jnp.float32)

            @pl.when((at >= far) & (at < n - 1))
            def _():
                sum_copy(1, side, group, item, me).wait_recv()
                total[part] += sums_in[1, group, item].astype(jnp.float32)

            @pl.when(at != far)
            def _():
                sums_out[group, item] = total[part].astype(jnp.bfloat16)

            @pl.when(at < far)
            def _():
                sum_copy(0, side, group, item, ahead[side]).start()

            @pl.when(at > far)
            def _():
                sum_copy(1, side, group, item, back[side]).start()

            @pl.when(at == far)
            def _():
                sums_out[group, item] = (
                    held[group, item].astype(jnp.float32) + total[part] + ob_ref[...]
                ).astype(jnp.bfloat16)
                leaves = (tick == TICKS - 1) | (following == 0)
                passes = (following == 0) & (home != me) & (tick < TICKS - 1)

                @pl.when(passes)
                def _():
                    pass_copy(side, group, item, tick, piece).start()

                @pl.when(leaves & jnp.logical_not(passes))
                def _():
                    final_copy(
                        sums_out.at[group, item], outgoing(side, item),
                        tick, piece, following, home,
                    ).start()

                @pl.when(jnp.logical_not(leaves))
                def _():
                    relay_copy(side, group, item).start()

    def pass_on(slot, side, settled):
        item, active = at_slot(slot, end_lag + PASS_LAG)
        tick, piece, home, group = place(sections - 1, side, item)

        @pl.when(
            active & (section == 0) & (places[side] == far) & (home != me) & (tick < TICKS - 1)
        )
        def _():
            copy = final_copy(
                passing.at[tick, piece], pass_send.at[piece], tick, piece, section, home
            )
            if settled:
                copy.wait_send()
            else:
                pass_copy(side, group, item, tick, piece).wait_recv()
                copy.start()

    def compute(slot):
        found = [at_slot(slot, lag) for lag in gather_lag]

        @pl.when(found[0][1] | found[1][1])
        def _():
            blocks = []
            for side in range(2):
                own, other = found[side], found[1 - side]
                group = jnp.where(
                    own[1],
                    place(section, side, own[0])[3],
                    place(section, 1 - side, other[0])[3],
                )
                blocks.append(held[group, jnp.where(own[1], own[0], other[0])])
            normed = normalize(
                jnp.concatenate(blocks, axis=0).astype(jnp.float32),
                gain_ref[...], shift_ref[...],
            )
            preact = lax.dot_general(
                normed, win_ref[...], (((1,), (1,)), ((), ())),
                preferred_element_type=jnp.float32,
            )
            hidden = activate(preact + ib_ref[...].astype(jnp.float32)).astype(jnp.bfloat16)
            total[...] = jnp.dot(hidden, wout_ref[...], preferred_element_type=jnp.float32)

        finish(slot, 0)
        finish(slot, 1)

    def settle(slot, side):
        item, active = at_slot(slot, spread_lag[side])

        @pl.when(active)
        def _():
            tick, piece, home, group = place(section, side, item)
            goes_back, goes_ahead = hands_on(side, (tick == 0) | (section == 0), home)

            @pl.when(goes_ahead)
            def _():
                forward_copy(1, side, group, item, me).wait_send()

            @pl.when(goes_back)
            def _():
                forward_copy(0, side, group, item, me).wait_send()

        summed, ready = at_slot(slot, gather_lag[side])

        @pl.when(ready)
        def _():
            sum_copy(0, side, 0, summed, me).wait_send()

    def turn(slot, carry):
        compute(slot)
        for side in range(2):
            settle(slot - SETTLE_LAG, side)
            receive(slot + 1, side)
        for side in range(2):
            pass_on(slot - SETTLE_LAG, side, True)
            pass_on(slot, side, False)
        return carry

    for side in range(2):
        receive(jnp.int32(0), side)
    for load in loads[1:7]:
        load.wait()
    lax.fori_loop(0, items + end_lag + SETTLE_LAG + PASS_LAG, turn, 0)

    def unship(tick):
        sends = me != (my_side if tick else my_start)
        if tick:
            sends = sends & (section == carriers[tick - 1])

        @pl.when(sends)
        def _():
            pltpu.make_async_remote_copy(
                src_ref=x_ref,
                dst_ref=o_ref.at[0],
                send_sem=ship_send.at[tick],
                recv_sem=final_recv.at[0],
                device_id={"section": section, "tensor": me},
                device_id_type=MESH,
            ).wait_send()

    def collect(tick):
        pltpu.make_async_remote_copy(
            src_ref=x_ref,
            dst_ref=o_ref.at[tick],
            send_sem=ship_send.at[0],
            recv_sem=final_recv.at[tick],
            device_id={"section": section, "tensor": me},
            device_id_type=MESH,
        ).wait_recv()

    unship(0)
    collect(TICKS - 1)

    @pl.when(carries)
    def _():
        for tick in range(1, TICKS):
            unship(tick)

    @pl.when(section == 0)
    def _():
        for tick in range(TICKS - 1):
            collect(tick)


def relay_call(n, sections, pieces, hop_slots, args):
    x, w_in, in_bias, w_out, out_bias, gain, shift, patches, plan = args
    tokens, width = x.shape
    rows = tokens // pieces
    chunks = n // 2 * pieces
    items = TICKS * chunks
    micro = patches.shape[0]
    bf16 = jnp.bfloat16
    vmem = pl.BlockSpec(memory_space=pltpu.VMEM)
    every = (2, items, rows, width)
    dma = pltpu.SemaphoreType.DMA
    out = pl.pallas_call(
        functools.partial(relay_kernel, n, sections, hop_slots),
        out_shape=pltpu.VMEM((TICKS, pieces, rows, width), bf16),
        in_specs=[pl.BlockSpec(memory_space=pl.ANY)] * 9,
        out_specs=vmem,
        scratch_shapes=[
            pltpu.VMEM((pieces, rows, width), bf16),
            pltpu.VMEM(w_in.shape, bf16),
            pltpu.VMEM((1, w_in.shape[0]), bf16),
            pltpu.VMEM(w_out.shape, bf16),
            pltpu.VMEM((1, width), jnp.float32),
            pltpu.VMEM((1, width), jnp.float32),
            pltpu.VMEM((1, width), jnp.float32),
            pltpu.VMEM((micro, pieces, rows, width), bf16),
            pltpu.SMEM(plan.shape, jnp.int32),
            dma((9,)),
            pltpu.VMEM(every, bf16),
            pltpu.VMEM((2,) + every, bf16),
            pltpu.VMEM(every, bf16),
            pltpu.VMEM((TICKS - 1, pieces, rows, width), bf16),
            pltpu.VMEM((TICKS - 1, pieces, rows, width), bf16),
            pltpu.VMEM((2 * rows, width), jnp.float32),
            dma((2, 2, SEND_RING)),
            dma((2, chunks)),
            dma((items - chunks,)),
            dma((2, SEND_RING)),
            dma((2, 2, chunks)),
            dma((TICKS,)),
            dma((pieces,)),
            dma((TICKS - 1, pieces)),
            dma((TICKS,)),
        ],
        compiler_params=pltpu.CompilerParams(
            collective_id=0, has_side_effects=True, vmem_limit_bytes=VMEM_BYTES
        ),
    )(
        x.reshape(pieces, rows, width),
        w_in,
        in_bias.reshape(1, -1),
        w_out,
        out_bias.reshape(1, -1),
        gain.reshape(1, -1),
        shift.reshape(1, -1),
        patches.reshape(micro, pieces, rows, width),
        plan,
    )
    return out.reshape(1, TICKS, tokens, width)


def passed_along(value, axis, steps):
    count = lax.axis_size(axis)
    pairs = [(source, (source + steps) % count) for source in range(count)]
    return lax.ppermute(value, axis, pairs)


def gathered_weights(args):
    current, w_in, in_bias, w_out, bias_row, gain_row, shift_row, patches, plan = args
    section_index = lax.axis_index("section")
    full_in, full_bias, full_out = (
        lax.all_gather(value, "tensor", axis=0, tiled=True) for value in (w_in, in_bias, w_out)
    )
    records = []
    for tick_index in range(TICKS):
        widened = current.astype(jnp.float32)
        normed = normalize(widened, gain_row, shift_row)
        preact = lax.dot_general(
            normed, full_in, (((1,), (1,)), ((), ())), preferred_element_type=jnp.float32
        )
        hidden = activate(preact + full_bias.astype(jnp.float32)).astype(jnp.bfloat16)
        produced = (
            widened + jnp.dot(hidden, full_out, preferred_element_type=jnp.float32) + bias_row
        ).astype(jnp.bfloat16)
        arrived = passed_along(produced, "section", 1)
        records.append(arrived)
        if tick_index + 1 < TICKS:
            selected = lax.dynamic_index_in_dim(patches, plan[tick_index], 0, keepdims=False)
            current = jnp.where(section_index == 0, selected, arrived)
    return jnp.stack(records, axis=0)[None]


def shards(n, sections, *blocks):
    args = tuple(block[0] for block in blocks[:7]) + blocks[7:]
    tokens, width = args[0].shape
    room = 2 * width * (
        tokens * (TICKS * (5 * n + 2) + 1 + args[7].shape[0]) + 2 * args[1].shape[0]
    )
    if tokens % (PIECES * 16) or n % 2 or sections < 2 or room > VMEM_BYTES * 3 // 4:
        return gathered_weights(args)
    return relay_call(n, sections, PIECES, HOP_SLOTS, args)


def solution(mesh):
    placed = (
        P("section", "tensor", None),
        P("section", "tensor", None),
        P("section", "tensor"),
        P("section", "tensor", None),
        P("section", None),
        P("section", None),
        P("section", None),
        P(None, "tensor", None),
        P(),
    )
    return jax.shard_map(
        functools.partial(shards, mesh.shape["tensor"], mesh.shape["section"]),
        mesh=mesh,
        in_specs=placed,
        out_specs=P("section", None, "tensor", None),
        check_vma=False,
    )
```

```python
import functools

import jax
import jax.numpy as jnp
from jax import lax
from jax.experimental import pallas as pl
from jax.experimental.pallas import tpu as pltpu
from jax.sharding import PartitionSpec as P

TICKS = 4
PIECES = 4
HOP_SLOTS = 2
SETTLE_LAG = 3
SEND_RING = 4
PASS_LAG = 1
VMEM_BYTES = 60 * 1024 * 1024

norm_floor = 0.1
gelu_slope = 1.702
MESH = pl.DeviceIdType.MESH


def activate(preact):
    return preact * jax.nn.sigmoid(gelu_slope * preact)


def normalize(widened, gain_row, shift_row):
    average = jnp.mean(widened, axis=-1, keepdims=True)
    centered = widened - average
    variance = jnp.mean(centered * centered, axis=-1, keepdims=True)
    return (centered * lax.rsqrt(variance + norm_floor) * gain_row + shift_row).astype(
        jnp.bfloat16
    )


def relay_kernel(
    n, sections, hop_slots,
    x_hbm, win_hbm, ib_hbm, wout_hbm, ob_hbm, gain_hbm, shift_hbm, patches_hbm, plan_hbm,
    o_ref,
    x_ref, win_ref, ib_ref, wout_ref, ob_ref, gain_ref, shift_ref, patches_ref, plan_ref,
    load_sem, held, sums_in, sums_out, staged, passing, total,
    x_send, x_recv, relay_recv, sum_send, sum_recv, ship_send, pass_send, pass_recv, final_recv,
):
    pieces, rows = x_hbm.shape[0], x_hbm.shape[1]
    near, far = n // 2 - 1, n // 2
    chunks = n // 2 * pieces
    items = TICKS * chunks
    me = lax.axis_index("tensor")
    section = lax.axis_index("section")
    following = lax.rem(section + 1, sections)
    preceding = lax.rem(section + sections - 1, sections)
    carriers = [(2 * tick + 1) % sections for tick in range(1, TICKS)]

    carries = section == 0
    for carrier in carriers:
        carries = carries | (section == carrier)

    def entry_side(origin):
        length = jnp.minimum(TICKS, sections - origin)
        return jnp.where(origin >= 0, lax.rem(length, 2), 0)

    def start_of(group, origin):
        return jnp.where(lax.rem(group + entry_side(origin), 2) == 0, near, far)

    my_group = jnp.where(me < n // 2, 0, 1)
    my_shard = jnp.where(me < n // 2, me, n - 1 - me)
    my_start = start_of(my_group, section)
    my_side = jnp.where(me < n // 2, near, far)

    barrier = pltpu.get_barrier_semaphore()

    def greet(sect, tensor):
        pl.semaphore_signal(
            barrier, inc=1, device_id={"section": sect, "tensor": tensor}, device_id_type=MESH
        )

    greet(following, me)
    greet(preceding, me)
    pl.when(me > 0)(lambda: greet(section, me - 1))
    pl.when(me < n - 1)(lambda: greet(section, me + 1))
    for home in range(n):
        group = home * 2 // n
        distant = jnp.abs(me - home) > 1
        pl.when(distant & (me == start_of(group, section)))(
            functools.partial(greet, section, home)
        )
        for carrier in carriers:
            if carrier and home != (near, far)[group]:
                pl.when((section == 0) & (me == (near, far)[group]))(
                    functools.partial(greet, carrier, home)
                )
    loads = [
        pltpu.make_async_copy(source, target, load_sem.at[index])
        for index, (source, target) in enumerate(
            [
                (x_hbm, x_ref), (gain_hbm, gain_ref), (shift_hbm, shift_ref),
                (win_hbm, win_ref), (ib_hbm, ib_ref), (wout_hbm, wout_ref),
                (ob_hbm, ob_ref), (plan_hbm, plan_ref), (patches_hbm, patches_ref),
            ]
        )
    ]
    for load in loads[:7]:
        load.start()

    @pl.when(carries)
    def _():
        for load in loads[7:]:
            load.start()

    expected = 4 - jnp.where((me == 0) | (me == n - 1), 1, 0)
    expected = expected + jnp.where(jnp.abs(me - my_start) > 1, 1, 0)
    for carrier in carriers:
        if carrier:
            expected = expected + jnp.where((section == carrier) & (me != my_side), 1, 0)
    pl.semaphore_wait(barrier, expected)

    def x_copy(src, group, item, sect, tensor, send_sem, recv_sem):
        return pltpu.make_async_remote_copy(
            src_ref=src,
            dst_ref=held.at[group, item],
            send_sem=send_sem,
            recv_sem=recv_sem,
            device_id={"section": sect, "tensor": tensor},
            device_id_type=MESH,
        )

    def spread_sem(group, item):
        return x_recv.at[group, lax.rem(item, chunks)]

    def forward_copy(way, side, group, item, tensor):
        return x_copy(
            held.at[group, item], group, item, section, tensor,
            x_send.at[way, side, lax.rem(item, SEND_RING)], spread_sem(group, item),
        )

    def outgoing(side, item):
        return sum_send.at[side, lax.rem(item, SEND_RING)]

    def relay_copy(side, group, item):
        return x_copy(
            sums_out.at[group, item], group, item + chunks, following, me,
            outgoing(side, item), relay_recv.at[item],
        )

    def sum_copy(way, side, group, item, tensor):
        return pltpu.make_async_remote_copy(
            src_ref=sums_out.at[group, item],
            dst_ref=sums_in.at[way, group, item],
            send_sem=outgoing(side, item),
            recv_sem=sum_recv.at[way, group, lax.rem(item, chunks)],
            device_id={"section": section, "tensor": tensor},
            device_id_type=MESH,
        )

    def final_copy(src, send_sem, tick, piece, sect, home):
        return pltpu.make_async_remote_copy(
            src_ref=src,
            dst_ref=o_ref.at[tick, piece],
            send_sem=send_sem,
            recv_sem=final_recv.at[tick],
            device_id={"section": sect, "tensor": home},
            device_id_type=MESH,
        )

    def pass_copy(side, group, item, tick, piece):
        return pltpu.make_async_remote_copy(
            src_ref=sums_out.at[group, item],
            dst_ref=passing.at[tick, piece],
            send_sem=outgoing(side, item),
            recv_sem=pass_recv.at[tick, piece],
            device_id={"section": following, "tensor": me},
            device_id_type=MESH,
        )

    places = (me, n - 1 - me)
    ahead = (me + 1, me - 1)
    back = (me - 1, me + 1)
    spread_lag = [
        jnp.where(at <= near, near - at, at - near) * hop_slots for at in places
    ]
    gather_lag = [
        jnp.where(at <= near, near + at, 2 * n - 2 - near - at) * hop_slots for at in places
    ]
    end_lag = (2 * n - 2 - near - far) * hop_slots

    def place(sect, side, item):
        tick, chunk = lax.div(item, chunks), lax.rem(item, chunks)
        shard, piece = lax.div(chunk, pieces), lax.rem(chunk, pieces)
        turns = jnp.minimum(tick, sect) + entry_side(sect - tick)
        group = lax.rem(turns + side, 2)
        home = jnp.where(group == 0, shard, n - 1 - shard)
        return tick, piece, home, group

    def enter(tick, piece, carry):
        item = tick * chunks + my_shard * pieces + piece
        source, start = x_ref.at[piece], my_start
        if tick:
            source, start = staged.at[tick - 1, piece], my_side
            staged[tick - 1, piece] = patches_ref[plan_ref[tick - 1], piece]
        if tick == 0:
            held[my_group, item] = source[...]
        else:

            @pl.when(section == 0)
            def _():
                held[my_group, item] = source[...]

        sends = me != start
        if tick:
            sends = sends & (section == carriers[tick - 1])

        @pl.when(sends)
        def _():
            sect = 0 if tick else section
            arrival = relay_recv.at[item - chunks] if tick else spread_sem(my_group, item)
            x_copy(
                source, my_group, item, sect, start, ship_send.at[tick], arrival
            ).start()

        return carry

    loads[0].wait()
    lax.fori_loop(0, pieces, functools.partial(enter, 0), 0)

    @pl.when(carries)
    def _():
        for load in loads[7:]:
            load.wait()
        for tick in range(1, TICKS):
            lax.fori_loop(0, pieces, functools.partial(enter, tick), 0)

    def at_slot(slot, lag):
        item = slot - lag
        return item, (item >= 0) & (item < items)

    def hands_on(side, entry, home):
        at = places[side]
        goes_back = (at > 0) & (at <= near) & jnp.logical_not(entry & (home == back[side]))
        goes_ahead = (
            (at >= near) & (at < n - 1) & jnp.logical_not(entry & (home == ahead[side]))
        )
        return goes_back, goes_ahead

    def receive(slot, side):
        item, active = at_slot(slot, spread_lag[side])

        @pl.when(active)
        def _():
            tick, piece, home, group = place(section, side, item)
            entry = (tick == 0) | (section == 0)

            arrives = jnp.logical_not(entry & (home == me))
            starts = (places[side] == near) & (tick > 0)

            @pl.when(arrives & starts)
            def _():
                relay_copy(side, group, item - chunks).wait_recv()

            @pl.when(arrives & jnp.logical_not(starts))
            def _():
                forward_copy(0, side, group, item, me).wait_recv()

            goes_back, goes_ahead = hands_on(side, entry, home)

            @pl.when(goes_ahead)
            def _():
                forward_copy(1, side, group, item, ahead[side]).start()

            @pl.when(goes_back)
            def _():
                forward_copy(0, side, group, item, back[side]).start()

            @pl.when((tick > 0) & (section > 0) & (home == me))
            def _():
                o_ref[tick - 1, piece] = held[group, item]

    def finish(slot, side):
        item, active = at_slot(slot, gather_lag[side])
        at = places[side]
        part = pl.ds(side * rows, rows)

        @pl.when(active)
        def _():
            tick, piece, home, group = place(section, side, item)

            @pl.when((at > 0) & (at <= far))
            def _():
                sum_copy(0, side, group, item, me).wait_recv()
                total[part] += sums_in[0, group, item].astype(jnp.float32)

            @pl.when((at >= far) & (at < n - 1))
            def _():
                sum_copy(1, side, group, item, me).wait_recv()
                total[part] += sums_in[1, group, item].astype(jnp.float32)

            @pl.when(at != far)
            def _():
                sums_out[group, item] = total[part].astype(jnp.bfloat16)

            @pl.when(at < far)
            def _():
                sum_copy(0, side, group, item, ahead[side]).start()

            @pl.when(at > far)
            def _():
                sum_copy(1, side, group, item, back[side]).start()

            @pl.when(at == far)
            def _():
                sums_out[group, item] = (
                    held[group, item].astype(jnp.float32) + total[part] + ob_ref[...]
                ).astype(jnp.bfloat16)
                leaves = (tick == TICKS - 1) | (following == 0)
                passes = (following == 0) & (home != me) & (tick < TICKS - 1)

                @pl.when(passes)
                def _():
                    pass_copy(side, group, item, tick, piece).start()

                @pl.when(leaves & jnp.logical_not(passes))
                def _():
                    final_copy(
                        sums_out.at[group, item], outgoing(side, item),
                        tick, piece, following, home,
                    ).start()

                @pl.when(jnp.logical_not(leaves))
                def _():
                    relay_copy(side, group, item).start()

    def pass_on(slot, side, settled):
        item, active = at_slot(slot, end_lag + PASS_LAG)
        tick, piece, home, group = place(sections - 1, side, item)

        @pl.when(
            active & (section == 0) & (places[side] == far) & (home != me) & (tick < TICKS - 1)
        )
        def _():
            copy = final_copy(
                passing.at[tick, piece], pass_send.at[piece], tick, piece, section, home
            )
            if settled:
                copy.wait_send()
            else:
                pass_copy(side, group, item, tick, piece).wait_recv()
                copy.start()

    def compute(slot):
        found = [at_slot(slot, lag) for lag in gather_lag]

        @pl.when(found[0][1] | found[1][1])
        def _():
            blocks = []
            for side in range(2):
                own, other = found[side], found[1 - side]
                group = jnp.where(
                    own[1],
                    place(section, side, own[0])[3],
                    place(section, 1 - side, other[0])[3],
                )
                blocks.append(held[group, jnp.where(own[1], own[0], other[0])])
            normed = normalize(
                jnp.concatenate(blocks, axis=0).astype(jnp.float32),
                gain_ref[...], shift_ref[...],
            )
            preact = lax.dot_general(
                normed, win_ref[...], (((1,), (1,)), ((), ())),
                preferred_element_type=jnp.float32,
            )
            hidden = activate(preact + ib_ref[...].astype(jnp.float32)).astype(jnp.bfloat16)
            total[...] = jnp.dot(hidden, wout_ref[...], preferred_element_type=jnp.float32)

        finish(slot, 0)
        finish(slot, 1)

    def settle(slot, side):
        item, active = at_slot(slot, spread_lag[side])

        @pl.when(active)
        def _():
            tick, piece, home, group = place(section, side, item)
            goes_back, goes_ahead = hands_on(side, (tick == 0) | (section == 0), home)

            @pl.when(goes_ahead)
            def _():
                forward_copy(1, side, group, item, me).wait_send()

            @pl.when(goes_back)
            def _():
                forward_copy(0, side, group, item, me).wait_send()

        summed, ready = at_slot(slot, gather_lag[side])

        @pl.when(ready)
        def _():
            sum_copy(0, side, 0, summed, me).wait_send()

    def turn(slot, carry):
        compute(slot)
        for side in range(2):
            settle(slot - SETTLE_LAG, side)
            receive(slot + 1, side)
        for side in range(2):
            pass_on(slot - SETTLE_LAG, side, True)
            pass_on(slot, side, False)
        return carry

    for side in range(2):
        receive(jnp.int32(0), side)
    for load in loads[1:7]:
        load.wait()
    lax.fori_loop(0, items + end_lag + SETTLE_LAG + PASS_LAG, turn, 0)

    def unship(tick):
        sends = me != (my_side if tick else my_start)
        if tick:
            sends = sends & (section == carriers[tick - 1])

        @pl.when(sends)
        def _():
            pltpu.make_async_remote_copy(
                src_ref=x_ref,
                dst_ref=o_ref.at[0],
                send_sem=ship_send.at[tick],
                recv_sem=final_recv.at[0],
                device_id={"section": section, "tensor": me},
                device_id_type=MESH,
            ).wait_send()

    def collect(tick):
        pltpu.make_async_remote_copy(
            src_ref=x_ref,
            dst_ref=o_ref.at[tick],
            send_sem=ship_send.at[0],
            recv_sem=final_recv.at[tick],
            device_id={"section": section, "tensor": me},
            device_id_type=MESH,
        ).wait_recv()

    unship(0)
    collect(TICKS - 1)

    @pl.when(carries)
    def _():
        for tick in range(1, TICKS):
            unship(tick)

    @pl.when(section == 0)
    def _():
        for tick in range(TICKS - 1):
            collect(tick)


def relay_call(n, sections, pieces, hop_slots, args):
    x, w_in, in_bias, w_out, out_bias, gain, shift, patches, plan = args
    tokens, width = x.shape
    rows = tokens // pieces
    chunks = n // 2 * pieces
    items = TICKS * chunks
    micro = patches.shape[0]
    bf16 = jnp.bfloat16
    vmem = pl.BlockSpec(memory_space=pltpu.VMEM)
    every = (2, items, rows, width)
    dma = pltpu.SemaphoreType.DMA
    out = pl.pallas_call(
        functools.partial(relay_kernel, n, sections, hop_slots),
        out_shape=pltpu.VMEM((TICKS, pieces, rows, width), bf16),
        in_specs=[pl.BlockSpec(memory_space=pl.ANY)] * 9,
        out_specs=vmem,
        scratch_shapes=[
            pltpu.VMEM((pieces, rows, width), bf16),
            pltpu.VMEM(w_in.shape, bf16),
            pltpu.VMEM((1, w_in.shape[0]), bf16),
            pltpu.VMEM(w_out.shape, bf16),
            pltpu.VMEM((1, width), jnp.float32),
            pltpu.VMEM((1, width), jnp.float32),
            pltpu.VMEM((1, width), jnp.float32),
            pltpu.VMEM((micro, pieces, rows, width), bf16),
            pltpu.SMEM(plan.shape, jnp.int32),
            dma((9,)),
            pltpu.VMEM(every, bf16),
            pltpu.VMEM((2,) + every, bf16),
            pltpu.VMEM(every, bf16),
            pltpu.VMEM((TICKS - 1, pieces, rows, width), bf16),
            pltpu.VMEM((TICKS - 1, pieces, rows, width), bf16),
            pltpu.VMEM((2 * rows, width), jnp.float32),
            dma((2, 2, SEND_RING)),
            dma((2, chunks)),
            dma((items - chunks,)),
            dma((2, SEND_RING)),
            dma((2, 2, chunks)),
            dma((TICKS,)),
            dma((pieces,)),
            dma((TICKS - 1, pieces)),
            dma((TICKS,)),
        ],
        compiler_params=pltpu.CompilerParams(
            collective_id=0, has_side_effects=True, vmem_limit_bytes=VMEM_BYTES
        ),
    )(
        x.reshape(pieces, rows, width),
        w_in,
        in_bias.reshape(1, -1),
        w_out,
        out_bias.reshape(1, -1),
        gain.reshape(1, -1),
        shift.reshape(1, -1),
        patches.reshape(micro, pieces, rows, width),
        plan,
    )
    return out.reshape(1, TICKS, tokens, width)


def passed_along(value, axis, steps):
    count = lax.axis_size(axis)
    pairs = [(source, (source + steps) % count) for source in range(count)]
    return lax.ppermute(value, axis, pairs)


def gathered_weights(args):
    current, w_in, in_bias, w_out, bias_row, gain_row, shift_row, patches, plan = args
    section_index = lax.axis_index("section")
    full_in, full_bias, full_out = (
        lax.all_gather(value, "tensor", axis=0, tiled=True) for value in (w_in, in_bias, w_out)
    )
    records = []
    for tick_index in range(TICKS):
        widened = current.astype(jnp.float32)
        normed = normalize(widened, gain_row, shift_row)
        preact = lax.dot_general(
            normed, full_in, (((1,), (1,)), ((), ())), preferred_element_type=jnp.float32
        )
        hidden = activate(preact + full_bias.astype(jnp.float32)).astype(jnp.bfloat16)
        produced = (
            widened + jnp.dot(hidden, full_out, preferred_element_type=jnp.float32) + bias_row
        ).astype(jnp.bfloat16)
        arrived = passed_along(produced, "section", 1)
        records.append(arrived)
        if tick_index + 1 < TICKS:
            selected = lax.dynamic_index_in_dim(patches, plan[tick_index], 0, keepdims=False)
            current = jnp.where(section_index == 0, selected, arrived)
    return jnp.stack(records, axis=0)[None]


def shards(n, sections, *blocks):
    args = tuple(block[0] for block in blocks[:7]) + blocks[7:]
    tokens, width = args[0].shape
    room = 2 * width * (
        tokens * (TICKS * (5 * n + 2) + 1 + args[7].shape[0]) + 2 * args[1].shape[0]
    )
    if tokens % (PIECES * 16) or n % 2 or sections < 2 or room > VMEM_BYTES * 3 // 4:
        return gathered_weights(args)
    return relay_call(n, sections, PIECES, HOP_SLOTS, args)


def solution(mesh):
    placed = (
        P("section", "tensor", None),
        P("section", "tensor", None),
        P("section", "tensor"),
        P("section", "tensor", None),
        P("section", None),
        P("section", None),
        P("section", None),
        P(None, "tensor", None),
        P(),
    )
    return jax.shard_map(
        functools.partial(shards, mesh.shape["tensor"], mesh.shape["section"]),
        mesh=mesh,
        in_specs=placed,
        out_specs=P("section", None, "tensor", None),
        check_vma=False,
    )
```

```python
import functools

import jax
import jax.numpy as jnp
from jax import lax
from jax.experimental import pallas as pl
from jax.experimental.pallas import tpu as pltpu
from jax.sharding import PartitionSpec as P

TICKS = 4
PIECES = 4
HOP_SLOTS = 2
SETTLE_LAG = 3
SEND_RING = 4
PASS_LAG = 1
VMEM_BYTES = 60 * 1024 * 1024

norm_floor = 0.1
gelu_slope = 1.702
MESH = pl.DeviceIdType.MESH


def activate(preact):
    return preact * jax.nn.sigmoid(gelu_slope * preact)


def normalize(widened, gain_row, shift_row):
    average = jnp.mean(widened, axis=-1, keepdims=True)
    centered = widened - average
    variance = jnp.mean(centered * centered, axis=-1, keepdims=True)
    return (centered * lax.rsqrt(variance + norm_floor) * gain_row + shift_row).astype(
        jnp.bfloat16
    )


def relay_kernel(
    n, sections, hop_slots,
    x_hbm, win_hbm, ib_hbm, wout_hbm, ob_hbm, gain_hbm, shift_hbm, patches_hbm, plan_hbm,
    o_ref,
    x_ref, win_ref, ib_ref, wout_ref, ob_ref, gain_ref, shift_ref, patches_ref, plan_ref,
    load_sem, held, sums_in, sums_out, staged, passing, kept, total,
    x_send, x_recv, relay_recv, sum_send, sum_recv, ship_send, pass_send, home_send, pass_recv, final_recv,
):
    pieces, rows = x_hbm.shape[0], x_hbm.shape[1]
    near, far = n // 2 - 1, n // 2
    chunks = n // 2 * pieces
    items = TICKS * chunks
    me = lax.axis_index("tensor")
    section = lax.axis_index("section")
    following = lax.rem(section + 1, sections)
    preceding = lax.rem(section + sections - 1, sections)
    carriers = [(2 * tick + 1) % sections for tick in range(1, TICKS)]

    carries = section == 0
    for carrier in carriers:
        carries = carries | (section == carrier)

    def entry_side(origin):
        length = jnp.minimum(TICKS, sections - origin)
        return jnp.where(origin >= 0, lax.rem(length, 2), 0)

    def start_of(group, origin):
        return jnp.where(lax.rem(group + entry_side(origin), 2) == 0, near, far)

    my_group = jnp.where(me < n // 2, 0, 1)
    my_shard = jnp.where(me < n // 2, me, n - 1 - me)
    my_start = start_of(my_group, section)
    my_side = jnp.where(me < n // 2, near, far)

    barrier = pltpu.get_barrier_semaphore()

    def greet(sect, tensor):
        pl.semaphore_signal(
            barrier, inc=1, device_id={"section": sect, "tensor": tensor}, device_id_type=MESH
        )

    greet(following, me)
    greet(preceding, me)
    pl.when(me > 0)(lambda: greet(section, me - 1))
    pl.when(me < n - 1)(lambda: greet(section, me + 1))
    for home in range(n):
        group = home * 2 // n
        distant = jnp.abs(me - home) > 1
        pl.when(distant & (me == start_of(group, section)))(
            functools.partial(greet, section, home)
        )
        for carrier in carriers:
            if carrier and home != (near, far)[group]:
                pl.when((section == 0) & (me == (near, far)[group]))(
                    functools.partial(greet, carrier, home)
                )
    loads = [
        pltpu.make_async_copy(source, target, load_sem.at[index])
        for index, (source, target) in enumerate(
            [
                (x_hbm, x_ref), (gain_hbm, gain_ref), (shift_hbm, shift_ref),
                (win_hbm, win_ref), (ib_hbm, ib_ref), (wout_hbm, wout_ref),
                (ob_hbm, ob_ref), (plan_hbm, plan_ref), (patches_hbm, patches_ref),
            ]
        )
    ]
    for load in loads[:7]:
        load.start()

    @pl.when(carries)
    def _():
        for load in loads[7:]:
            load.start()

    expected = 4 - jnp.where((me == 0) | (me == n - 1), 1, 0)
    expected = expected + jnp.where(jnp.abs(me - my_start) > 1, 1, 0)
    for carrier in carriers:
        if carrier:
            expected = expected + jnp.where((section == carrier) & (me != my_side), 1, 0)
    pl.semaphore_wait(barrier, expected)

    def x_copy(src, group, item, sect, tensor, send_sem, recv_sem):
        return pltpu.make_async_remote_copy(
            src_ref=src,
            dst_ref=held.at[group, item],
            send_sem=send_sem,
            recv_sem=recv_sem,
            device_id={"section": sect, "tensor": tensor},
            device_id_type=MESH,
        )

    def spread_sem(group, item):
        return x_recv.at[group, lax.rem(item, chunks)]

    def forward_copy(way, side, group, item, tensor):
        return x_copy(
            held.at[group, item], group, item, section, tensor,
            x_send.at[way, side, lax.rem(item, SEND_RING)], spread_sem(group, item),
        )

    def outgoing(side, item):
        return sum_send.at[side, lax.rem(item, SEND_RING)]

    def relay_copy(side, group, item):
        return x_copy(
            sums_out.at[group, item], group, item + chunks, following, me,
            outgoing(side, item), relay_recv.at[item],
        )

    def sum_copy(way, side, group, item, tensor):
        return pltpu.make_async_remote_copy(
            src_ref=sums_out.at[group, item],
            dst_ref=sums_in.at[way, group, item],
            send_sem=outgoing(side, item),
            recv_sem=sum_recv.at[way, group, lax.rem(item, chunks)],
            device_id={"section": section, "tensor": tensor},
            device_id_type=MESH,
        )

    def final_copy(src, send_sem, tick, piece, sect, home):
        return pltpu.make_async_remote_copy(
            src_ref=src,
            dst_ref=o_ref.at[tick, piece],
            send_sem=send_sem,
            recv_sem=final_recv.at[tick],
            device_id={"section": sect, "tensor": home},
            device_id_type=MESH,
        )

    def pass_copy(side, group, item, tick, piece):
        return pltpu.make_async_remote_copy(
            src_ref=sums_out.at[group, item],
            dst_ref=passing.at[tick, piece],
            send_sem=outgoing(side, item),
            recv_sem=pass_recv.at[tick, piece],
            device_id={"section": following, "tensor": me},
            device_id_type=MESH,
        )

    places = (me, n - 1 - me)
    ahead = (me + 1, me - 1)
    back = (me - 1, me + 1)
    spread_lag = [
        jnp.where(at <= near, near - at, at - near) * hop_slots for at in places
    ]
    gather_lag = [
        jnp.where(at <= near, near + at, 2 * n - 2 - near - at) * hop_slots for at in places
    ]
    end_lag = (2 * n - 2 - near - far) * hop_slots

    def place(sect, side, item):
        tick, chunk = lax.div(item, chunks), lax.rem(item, chunks)
        shard, piece = lax.div(chunk, pieces), lax.rem(chunk, pieces)
        turns = jnp.minimum(tick, sect) + entry_side(sect - tick)
        group = lax.rem(turns + side, 2)
        home = jnp.where(group == 0, shard, n - 1 - shard)
        return tick, piece, home, group

    def enter(tick, piece, carry):
        item = tick * chunks + my_shard * pieces + piece
        source, start = x_ref.at[piece], my_start
        if tick:
            source, start = staged.at[tick - 1, piece], my_side
            staged[tick - 1, piece] = patches_ref[plan_ref[tick - 1], piece]
        if tick == 0:
            held[my_group, item] = source[...]
        else:

            @pl.when(section == 0)
            def _():
                held[my_group, item] = source[...]

        sends = me != start
        if tick:
            sends = sends & (section == carriers[tick - 1])

        @pl.when(sends)
        def _():
            sect = 0 if tick else section
            arrival = relay_recv.at[item - chunks] if tick else spread_sem(my_group, item)
            x_copy(
                source, my_group, item, sect, start, ship_send.at[tick], arrival
            ).start()

        return carry

    loads[0].wait()
    lax.fori_loop(0, pieces, functools.partial(enter, 0), 0)

    @pl.when(carries)
    def _():
        for load in loads[7:]:
            load.wait()
        for tick in range(1, TICKS):
            lax.fori_loop(0, pieces, functools.partial(enter, tick), 0)

    def at_slot(slot, lag):
        item = slot - lag
        return item, (item >= 0) & (item < items)

    def hands_on(side, entry, home):
        at = places[side]
        goes_back = (at > 0) & (at <= near) & jnp.logical_not(entry & (home == back[side]))
        goes_ahead = (
            (at >= near) & (at < n - 1) & jnp.logical_not(entry & (home == ahead[side]))
        )
        return goes_back, goes_ahead

    def receive(slot, side):
        item, active = at_slot(slot, spread_lag[side])

        @pl.when(active)
        def _():
            tick, piece, home, group = place(section, side, item)
            entry = (tick == 0) | (section == 0)

            arrives = jnp.logical_not(entry & (home == me))
            starts = (places[side] == near) & (tick > 0)

            @pl.when(arrives & starts)
            def _():
                relay_copy(side, group, item - chunks).wait_recv()

            @pl.when(arrives & jnp.logical_not(starts))
            def _():
                forward_copy(0, side, group, item, me).wait_recv()

            goes_back, goes_ahead = hands_on(side, entry, home)

            @pl.when(goes_ahead)
            def _():
                forward_copy(1, side, group, item, ahead[side]).start()

            @pl.when(goes_back)
            def _():
                forward_copy(0, side, group, item, back[side]).start()

            @pl.when((tick > 0) & (section > 0) & (home == me))
            def _():
                o_ref[tick - 1, piece] = held[group, item]

    def finish(slot, side):
        item, active = at_slot(slot, gather_lag[side])
        at = places[side]
        part = pl.ds(side * rows, rows)

        @pl.when(active)
        def _():
            tick, piece, home, group = place(section, side, item)

            @pl.when((at > 0) & (at <= far))
            def _():
                sum_copy(0, side, group, item, me).wait_recv()
                total[part] += sums_in[0, group, item].astype(jnp.float32)

            homing = (tick == TICKS - 1) & (jnp.int32(far + 1) == n - 1)
            turning = homing & (at == far) & (home == ahead[side])
            ending = homing & (at == n - 1) & (home == me)

            @pl.when((at >= far) & (at < n - 1) & jnp.logical_not(turning))
            def _():
                sum_copy(1, side, group, item, me).wait_recv()
                total[part] += sums_in[1, group, item].astype(jnp.float32)

            @pl.when(ending)
            def _():
                kept[piece] = held[group, item].astype(jnp.float32) + total[part] + ob_ref[...]

            @pl.when(((at != far) | turning) & jnp.logical_not(ending))
            def _():
                sums_out[group, item] = total[part].astype(jnp.bfloat16)

            @pl.when((at < far) | turning)
            def _():
                sum_copy(0, side, group, item, ahead[side]).start()

            @pl.when((at > far) & jnp.logical_not(ending))
            def _():
                sum_copy(1, side, group, item, back[side]).start()

            @pl.when((at == far) & jnp.logical_not(turning))
            def _():
                sums_out[group, item] = (
                    held[group, item].astype(jnp.float32) + total[part] + ob_ref[...]
                ).astype(jnp.bfloat16)
                leaves = (tick == TICKS - 1) | (following == 0)
                passes = (following == 0) & (home != me) & (tick < TICKS - 1)

                @pl.when(passes)
                def _():
                    pass_copy(side, group, item, tick, piece).start()

                @pl.when(leaves & jnp.logical_not(passes))
                def _():
                    final_copy(
                        sums_out.at[group, item], outgoing(side, item),
                        tick, piece, following, home,
                    ).start()

                @pl.when(jnp.logical_not(leaves))
                def _():
                    relay_copy(side, group, item).start()

    def end_home(slot, side):
        item, active = at_slot(slot, end_lag + hop_slots)
        tick, piece, home, group = place(section, side, item)
        last = (tick == TICKS - 1) & (jnp.int32(far + 1) == n - 1)

        @pl.when(active & last & (places[side] == n - 1) & (home == me))
        def _():
            sum_copy(0, side, group, item, me).wait_recv()
            sums_out[group, item] = (
                kept[piece] + sums_in[0, group, item].astype(jnp.float32)
            ).astype(jnp.bfloat16)
            final_copy(
                sums_out.at[group, item], home_send, tick, piece, following, me
            ).start()

    def pass_on(slot, side, settled):
        item, active = at_slot(slot, end_lag + PASS_LAG)
        tick, piece, home, group = place(sections - 1, side, item)

        @pl.when(
            active & (section == 0) & (places[side] == far) & (home != me) & (tick < TICKS - 1)
        )
        def _():
            copy = final_copy(
                passing.at[tick, piece], pass_send.at[piece], tick, piece, section, home
            )
            if settled:
                copy.wait_send()
            else:
                pass_copy(side, group, item, tick, piece).wait_recv()
                copy.start()

    def compute(slot):
        found = [at_slot(slot, lag) for lag in gather_lag]

        @pl.when(found[0][1] | found[1][1])
        def _():
            blocks = []
            for side in range(2):
                own, other = found[side], found[1 - side]
                group = jnp.where(
                    own[1],
                    place(section, side, own[0])[3],
                    place(section, 1 - side, other[0])[3],
                )
                blocks.append(held[group, jnp.where(own[1], own[0], other[0])])
            normed = normalize(
                jnp.concatenate(blocks, axis=0).astype(jnp.float32),
                gain_ref[...], shift_ref[...],
            )
            preact = lax.dot_general(
                normed, win_ref[...], (((1,), (1,)), ((), ())),
                preferred_element_type=jnp.float32,
            )
            hidden = activate(preact + ib_ref[...].astype(jnp.float32)).astype(jnp.bfloat16)
            total[...] = jnp.dot(hidden, wout_ref[...], preferred_element_type=jnp.float32)

    def settle(slot, side):
        item, active = at_slot(slot, spread_lag[side])

        @pl.when(active)
        def _():
            tick, piece, home, group = place(section, side, item)
            goes_back, goes_ahead = hands_on(side, (tick == 0) | (section == 0), home)

            @pl.when(goes_ahead)
            def _():
                forward_copy(1, side, group, item, me).wait_send()

            @pl.when(goes_back)
            def _():
                forward_copy(0, side, group, item, me).wait_send()

        summed, ready = at_slot(slot, gather_lag[side])

        @pl.when(ready)
        def _():
            tick, _, home, _ = place(section, side, summed)
            ending = (
                (tick == TICKS - 1) & (jnp.int32(far + 1) == n - 1)
                & (places[side] == n - 1) & (home == me)
            )

            @pl.when(jnp.logical_not(ending))
            def _():
                sum_copy(0, side, 0, summed, me).wait_send()

    def turn(slot, carry):
        compute(slot)
        for side in range(2):
            finish(slot, side)
            settle(slot - SETTLE_LAG, side)
            receive(slot + 1, side)
        for side in range(2):
            end_home(slot, side)
        for side in range(2):
            pass_on(slot - SETTLE_LAG, side, True)
            pass_on(slot, side, False)
        return carry

    for side in range(2):
        receive(jnp.int32(0), side)
    for load in loads[1:7]:
        load.wait()
    lax.fori_loop(0, items + end_lag + SETTLE_LAG + PASS_LAG, turn, 0)

    def unship(tick):
        sends = me != (my_side if tick else my_start)
        if tick:
            sends = sends & (section == carriers[tick - 1])

        @pl.when(sends)
        def _():
            pltpu.make_async_remote_copy(
                src_ref=x_ref,
                dst_ref=o_ref.at[0],
                send_sem=ship_send.at[tick],
                recv_sem=final_recv.at[0],
                device_id={"section": section, "tensor": me},
                device_id_type=MESH,
            ).wait_send()

    last_turns = jnp.minimum(TICKS - 1, section) + entry_side(section - TICKS + 1)
    my_end = lax.rem(my_group + last_turns, 2)

    @pl.when((jnp.int32(far + 1) == n - 1) & (jnp.where(my_end == 0, me, n - 1 - me) == n - 1))
    def _():
        pltpu.make_async_remote_copy(
            src_ref=x_ref,
            dst_ref=o_ref.at[0],
            send_sem=home_send,
            recv_sem=final_recv.at[0],
            device_id={"section": section, "tensor": me},
            device_id_type=MESH,
        ).wait_send()

    def collect(tick):
        pltpu.make_async_remote_copy(
            src_ref=x_ref,
            dst_ref=o_ref.at[tick],
            send_sem=ship_send.at[0],
            recv_sem=final_recv.at[tick],
            device_id={"section": section, "tensor": me},
            device_id_type=MESH,
        ).wait_recv()

    unship(0)
    collect(TICKS - 1)

    @pl.when(carries)
    def _():
        for tick in range(1, TICKS):
            unship(tick)

    @pl.when(section == 0)
    def _():
        for tick in range(TICKS - 1):
            collect(tick)


def relay_call(n, sections, pieces, hop_slots, args):
    x, w_in, in_bias, w_out, out_bias, gain, shift, patches, plan = args
    tokens, width = x.shape
    rows = tokens // pieces
    chunks = n // 2 * pieces
    items = TICKS * chunks
    micro = patches.shape[0]
    bf16 = jnp.bfloat16
    vmem = pl.BlockSpec(memory_space=pltpu.VMEM)
    every = (2, items, rows, width)
    dma = pltpu.SemaphoreType.DMA
    out = pl.pallas_call(
        functools.partial(relay_kernel, n, sections, hop_slots),
        out_shape=pltpu.VMEM((TICKS, pieces, rows, width), bf16),
        in_specs=[pl.BlockSpec(memory_space=pl.ANY)] * 9,
        out_specs=vmem,
        scratch_shapes=[
            pltpu.VMEM((pieces, rows, width), bf16),
            pltpu.VMEM(w_in.shape, bf16),
            pltpu.VMEM((1, w_in.shape[0]), bf16),
            pltpu.VMEM(w_out.shape, bf16),
            pltpu.VMEM((1, width), jnp.float32),
            pltpu.VMEM((1, width), jnp.float32),
            pltpu.VMEM((1, width), jnp.float32),
            pltpu.VMEM((micro, pieces, rows, width), bf16),
            pltpu.SMEM(plan.shape, jnp.int32),
            dma((9,)),
            pltpu.VMEM(every, bf16),
            pltpu.VMEM((2,) + every, bf16),
            pltpu.VMEM(every, bf16),
            pltpu.VMEM((TICKS - 1, pieces, rows, width), bf16),
            pltpu.VMEM((TICKS - 1, pieces, rows, width), bf16),
            pltpu.VMEM((pieces, rows, width), jnp.float32),
            pltpu.VMEM((2 * rows, width), jnp.float32),
            dma((2, 2, SEND_RING)),
            dma((2, chunks)),
            dma((items - chunks,)),
            dma((2, SEND_RING)),
            dma((2, 2, chunks)),
            dma((TICKS,)),
            dma((pieces,)),
            dma,
            dma((TICKS - 1, pieces)),
            dma((TICKS,)),
        ],
        compiler_params=pltpu.CompilerParams(
            collective_id=0, has_side_effects=True, vmem_limit_bytes=VMEM_BYTES
        ),
    )(
        x.reshape(pieces, rows, width),
        w_in,
        in_bias.reshape(1, -1),
        w_out,
        out_bias.reshape(1, -1),
        gain.reshape(1, -1),
        shift.reshape(1, -1),
        patches.reshape(micro, pieces, rows, width),
        plan,
    )
    return out.reshape(1, TICKS, tokens, width)


def passed_along(value, axis, steps):
    count = lax.axis_size(axis)
    pairs = [(source, (source + steps) % count) for source in range(count)]
    return lax.ppermute(value, axis, pairs)


def gathered_weights(args):
    current, w_in, in_bias, w_out, bias_row, gain_row, shift_row, patches, plan = args
    section_index = lax.axis_index("section")
    full_in, full_bias, full_out = (
        lax.all_gather(value, "tensor", axis=0, tiled=True) for value in (w_in, in_bias, w_out)
    )
    records = []
    for tick_index in range(TICKS):
        widened = current.astype(jnp.float32)
        normed = normalize(widened, gain_row, shift_row)
        preact = lax.dot_general(
            normed, full_in, (((1,), (1,)), ((), ())), preferred_element_type=jnp.float32
        )
        hidden = activate(preact + full_bias.astype(jnp.float32)).astype(jnp.bfloat16)
        produced = (
            widened + jnp.dot(hidden, full_out, preferred_element_type=jnp.float32) + bias_row
        ).astype(jnp.bfloat16)
        arrived = passed_along(produced, "section", 1)
        records.append(arrived)
        if tick_index + 1 < TICKS:
            selected = lax.dynamic_index_in_dim(patches, plan[tick_index], 0, keepdims=False)
            current = jnp.where(section_index == 0, selected, arrived)
    return jnp.stack(records, axis=0)[None]


def shards(n, sections, *blocks):
    args = tuple(block[0] for block in blocks[:7]) + blocks[7:]
    tokens, width = args[0].shape
    room = 2 * width * (
        tokens * (TICKS * (5 * n + 2) + 1 + args[7].shape[0]) + 2 * args[1].shape[0]
    )
    if tokens % (PIECES * 16) or n % 2 or sections < 2 or room > VMEM_BYTES * 3 // 4:
        return gathered_weights(args)
    return relay_call(n, sections, PIECES, HOP_SLOTS, args)


def solution(mesh):
    placed = (
        P("section", "tensor", None),
        P("section", "tensor", None),
        P("section", "tensor"),
        P("section", "tensor", None),
        P("section", None),
        P("section", None),
        P("section", None),
        P(None, "tensor", None),
        P(),
    )
    return jax.shard_map(
        functools.partial(shards, mesh.shape["tensor"], mesh.shape["section"]),
        mesh=mesh,
        in_specs=placed,
        out_specs=P("section", None, "tensor", None),
        check_vma=False,
    )
```

```python
import functools

import jax
import jax.numpy as jnp
from jax import lax
from jax.experimental import pallas as pl
from jax.experimental.pallas import tpu as pltpu
from jax.sharding import PartitionSpec as P

TICKS = 4
PIECES = 4
HOP_SLOTS = 2
SETTLE_LAG = 3
SEND_RING = 4
PASS_LAG = 1
VMEM_BYTES = 60 * 1024 * 1024

norm_floor = 0.1
gelu_slope = 1.702
MESH = pl.DeviceIdType.MESH


def activate(preact):
    return preact * jax.nn.sigmoid(gelu_slope * preact)


def normalize(widened, gain_row, shift_row):
    average = jnp.mean(widened, axis=-1, keepdims=True)
    centered = widened - average
    variance = jnp.mean(centered * centered, axis=-1, keepdims=True)
    return (centered * lax.rsqrt(variance + norm_floor) * gain_row + shift_row).astype(
        jnp.bfloat16
    )


def relay_kernel(
    n, sections, hop_slots,
    x_hbm, win_hbm, ib_hbm, wout_hbm, ob_hbm, gain_hbm, shift_hbm, patches_hbm, plan_hbm,
    o_ref,
    x_ref, win_ref, ib_ref, wout_ref, ob_ref, gain_ref, shift_ref, patches_ref, plan_ref,
    load_sem, held, sums_in, sums_out, staged, passing, total,
    x_send, x_recv, relay_recv, sum_send, sum_recv, ship_send, pass_send, pass_recv, final_recv,
):
    pieces, rows = x_hbm.shape[0], x_hbm.shape[1]
    near, far = n // 2 - 1, n // 2
    chunks = n // 2 * pieces
    items = TICKS * chunks
    me = lax.axis_index("tensor")
    section = lax.axis_index("section")
    following = lax.rem(section + 1, sections)
    preceding = lax.rem(section + sections - 1, sections)
    carriers = [(2 * tick + 1) % sections for tick in range(1, TICKS)]

    carries = section == 0
    for carrier in carriers:
        carries = carries | (section == carrier)

    def entry_side(origin):
        length = jnp.minimum(TICKS, sections - origin)
        return jnp.where(origin >= 0, lax.rem(length, 2), 0)

    def start_of(group, origin):
        return jnp.where(lax.rem(group + entry_side(origin), 2) == 0, near, far)

    my_group = jnp.where(me < n // 2, 0, 1)
    my_shard = jnp.where(me < n // 2, me, n - 1 - me)
    my_start = start_of(my_group, section)
    my_side = jnp.where(me < n // 2, near, far)

    barrier = pltpu.get_barrier_semaphore()

    def greet(sect, tensor):
        pl.semaphore_signal(
            barrier, inc=1, device_id={"section": sect, "tensor": tensor}, device_id_type=MESH
        )

    greet(following, me)
    greet(preceding, me)
    pl.when(me > 0)(lambda: greet(section, me - 1))
    pl.when(me < n - 1)(lambda: greet(section, me + 1))
    for home in range(n):
        group = home * 2 // n
        distant = jnp.abs(me - home) > 1
        pl.when(distant & (me == start_of(group, section)))(
            functools.partial(greet, section, home)
        )
        for carrier in carriers:
            if carrier and home != (near, far)[group]:
                pl.when((section == 0) & (me == (near, far)[group]))(
                    functools.partial(greet, carrier, home)
                )
    loads = [
        pltpu.make_async_copy(source, target, load_sem.at[index])
        for index, (source, target) in enumerate(
            [
                (x_hbm, x_ref), (gain_hbm, gain_ref), (shift_hbm, shift_ref),
                (win_hbm, win_ref), (ib_hbm, ib_ref), (wout_hbm, wout_ref),
                (ob_hbm, ob_ref), (plan_hbm, plan_ref), (patches_hbm, patches_ref),
            ]
        )
    ]
    for load in loads[:7]:
        load.start()

    @pl.when(carries)
    def _():
        for load in loads[7:]:
            load.start()

    expected = 4 - jnp.where((me == 0) | (me == n - 1), 1, 0)
    expected = expected + jnp.where(jnp.abs(me - my_start) > 1, 1, 0)
    for carrier in carriers:
        if carrier:
            expected = expected + jnp.where((section == carrier) & (me != my_side), 1, 0)
    pl.semaphore_wait(barrier, expected)

    def x_copy(src, group, item, sect, tensor, send_sem, recv_sem):
        return pltpu.make_async_remote_copy(
            src_ref=src,
            dst_ref=held.at[group, item],
            send_sem=send_sem,
            recv_sem=recv_sem,
            device_id={"section": sect, "tensor": tensor},
            device_id_type=MESH,
        )

    def spread_sem(group, item):
        return x_recv.at[group, lax.rem(item, chunks)]

    def forward_copy(way, side, group, item, tensor):
        return x_copy(
            held.at[group, item], group, item, section, tensor,
            x_send.at[way, side, lax.rem(item, SEND_RING)], spread_sem(group, item),
        )

    def outgoing(side, item):
        return sum_send.at[side, lax.rem(item, SEND_RING)]

    def relay_copy(side, group, item):
        return x_copy(
            sums_out.at[group, item], group, item + chunks, following, me,
            outgoing(side, item), relay_recv.at[item],
        )

    def sum_copy(way, side, group, item, tensor):
        return pltpu.make_async_remote_copy(
            src_ref=sums_out.at[group, item],
            dst_ref=sums_in.at[way, group, item],
            send_sem=outgoing(side, item),
            recv_sem=sum_recv.at[way, group, lax.rem(item, chunks)],
            device_id={"section": section, "tensor": tensor},
            device_id_type=MESH,
        )

    def final_copy(src, send_sem, tick, piece, sect, home):
        return pltpu.make_async_remote_copy(
            src_ref=src,
            dst_ref=o_ref.at[tick, piece],
            send_sem=send_sem,
            recv_sem=final_recv.at[tick],
            device_id={"section": sect, "tensor": home},
            device_id_type=MESH,
        )

    def pass_copy(side, group, item, tick, piece):
        return pltpu.make_async_remote_copy(
            src_ref=sums_out.at[group, item],
            dst_ref=passing.at[tick, piece],
            send_sem=outgoing(side, item),
            recv_sem=pass_recv.at[tick, piece],
            device_id={"section": following, "tensor": me},
            device_id_type=MESH,
        )

    places = (me, n - 1 - me)
    ahead = (me + 1, me - 1)
    back = (me - 1, me + 1)
    spread_lag = [
        jnp.where(at <= near, near - at, at - near) * hop_slots for at in places
    ]
    gather_lag = [
        jnp.where(at <= near, near + at, 2 * n - 2 - near - at) * hop_slots for at in places
    ]
    end_lag = (2 * n - 2 - near - far) * hop_slots

    def place(sect, side, item):
        tick, chunk = lax.div(item, chunks), lax.rem(item, chunks)
        shard, piece = lax.div(chunk, pieces), lax.rem(chunk, pieces)
        turns = jnp.minimum(tick, sect) + entry_side(sect - tick)
        group = lax.rem(turns + side, 2)
        home = jnp.where(group == 0, shard, n - 1 - shard)
        return tick, piece, home, group

    def enter(tick, piece, carry):
        item = tick * chunks + my_shard * pieces + piece
        source, start = x_ref.at[piece], my_start
        if tick:
            source, start = staged.at[tick - 1, piece], my_side
            staged[tick - 1, piece] = patches_ref[plan_ref[tick - 1], piece]
        if tick == 0:
            held[my_group, item] = source[...]
        else:

            @pl.when(section == 0)
            def _():
                held[my_group, item] = source[...]

        sends = me != start
        if tick:
            sends = sends & (section == carriers[tick - 1])

        @pl.when(sends)
        def _():
            sect = 0 if tick else section
            arrival = relay_recv.at[item - chunks] if tick else spread_sem(my_group, item)
            x_copy(
                source, my_group, item, sect, start, ship_send.at[tick], arrival
            ).start()

        return carry

    loads[0].wait()
    lax.fori_loop(0, pieces, functools.partial(enter, 0), 0)

    @pl.when(carries)
    def _():
        for load in loads[7:]:
            load.wait()
        for tick in range(1, TICKS):
            lax.fori_loop(0, pieces, functools.partial(enter, tick), 0)

    def at_slot(slot, lag):
        item = slot - lag
        return item, (item >= 0) & (item < items)

    def hands_on(side, entry, home):
        at = places[side]
        goes_back = (at > 0) & (at <= near) & jnp.logical_not(entry & (home == back[side]))
        goes_ahead = (
            (at >= near) & (at < n - 1) & jnp.logical_not(entry & (home == ahead[side]))
        )
        return goes_back, goes_ahead

    def receive(slot, side):
        item, active = at_slot(slot, spread_lag[side])

        @pl.when(active)
        def _():
            tick, piece, home, group = place(section, side, item)
            entry = (tick == 0) | (section == 0)

            arrives = jnp.logical_not(entry & (home == me))
            starts = (places[side] == near) & (tick > 0)

            @pl.when(arrives & starts)
            def _():
                relay_copy(side, group, item - chunks).wait_recv()

            @pl.when(arrives & jnp.logical_not(starts))
            def _():
                forward_copy(0, side, group, item, me).wait_recv()

            goes_back, goes_ahead = hands_on(side, entry, home)

            @pl.when(goes_ahead)
            def _():
                forward_copy(1, side, group, item, ahead[side]).start()

            @pl.when(goes_back)
            def _():
                forward_copy(0, side, group, item, back[side]).start()

            @pl.when((tick > 0) & (section > 0) & (home == me))
            def _():
                o_ref[tick - 1, piece] = held[group, item]

    def finish(slot, side):
        item, active = at_slot(slot, gather_lag[side])
        at = places[side]
        part = pl.ds(side * rows, rows)

        @pl.when(active)
        def _():
            tick, piece, home, group = place(section, side, item)

            @pl.when((at > 0) & (at <= far))
            def _():
                sum_copy(0, side, group, item, me).wait_recv()
                total[part] += sums_in[0, group, item].astype(jnp.float32)

            @pl.when((at >= far) & (at < n - 1))
            def _():
                sum_copy(1, side, group, item, me).wait_recv()
                total[part] += sums_in[1, group, item].astype(jnp.float32)

            @pl.when(at != far)
            def _():
                sums_out[group, item] = total[part].astype(jnp.bfloat16)

            @pl.when(at < far)
            def _():
                sum_copy(0, side, group, item, ahead[side]).start()

            @pl.when(at > far)
            def _():
                sum_copy(1, side, group, item, back[side]).start()

            @pl.when(at == far)
            def _():
                sums_out[group, item] = (
                    held[group, item].astype(jnp.float32) + total[part] + ob_ref[...]
                ).astype(jnp.bfloat16)
                leaves = (tick == TICKS - 1) | (following == 0)
                passes = (following == 0) & (home != me) & (tick < TICKS - 1)

                @pl.when(passes)
                def _():
                    pass_copy(side, group, item, tick, piece).start()

                @pl.when(leaves & jnp.logical_not(passes))
                def _():
                    final_copy(
                        sums_out.at[group, item], outgoing(side, item),
                        tick, piece, following, home,
                    ).start()

                @pl.when(jnp.logical_not(leaves))
                def _():
                    relay_copy(side, group, item).start()

    def pass_on(slot, side, settled):
        item, active = at_slot(slot, end_lag + PASS_LAG)
        tick, piece, home, group = place(sections - 1, side, item)

        @pl.when(
            active & (section == 0) & (places[side] == far) & (home != me) & (tick < TICKS - 1)
        )
        def _():
            copy = final_copy(
                passing.at[tick, piece], pass_send.at[piece], tick, piece, section, home
            )
            if settled:
                copy.wait_send()
            else:
                pass_copy(side, group, item, tick, piece).wait_recv()
                copy.start()

    def compute(slot):
        found = [at_slot(slot, lag) for lag in gather_lag]

        @pl.when(found[0][1] | found[1][1])
        def _():
            blocks = []
            for side in range(2):
                own, other = found[side], found[1 - side]
                group = jnp.where(
                    own[1],
                    place(section, side, own[0])[3],
                    place(section, 1 - side, other[0])[3],
                )
                blocks.append(held[group, jnp.where(own[1], own[0], other[0])])
            normed = normalize(
                jnp.concatenate(blocks, axis=0).astype(jnp.float32),
                gain_ref[...], shift_ref[...],
            )
            preact = lax.dot_general(
                normed, win_ref[...], (((1,), (1,)), ((), ())),
                preferred_element_type=jnp.float32,
            )
            hidden = activate(preact + ib_ref[...].astype(jnp.float32)).astype(jnp.bfloat16)
            total[...] = jnp.dot(hidden, wout_ref[...], preferred_element_type=jnp.float32)

        finish(slot, 0)
        finish(slot, 1)

    def settle(slot, side):
        item, active = at_slot(slot, spread_lag[side])

        @pl.when(active)
        def _():
            tick, piece, home, group = place(section, side, item)
            goes_back, goes_ahead = hands_on(side, (tick == 0) | (section == 0), home)

            @pl.when(goes_ahead)
            def _():
                forward_copy(1, side, group, item, me).wait_send()

            @pl.when(goes_back)
            def _():
                forward_copy(0, side, group, item, me).wait_send()

        summed, ready = at_slot(slot, gather_lag[side])

        @pl.when(ready)
        def _():
            sum_copy(0, side, 0, summed, me).wait_send()

    def turn(slot, carry):
        compute(slot)
        for side in range(2):
            settle(slot - SETTLE_LAG, side)
            receive(slot + 1, side)
        for side in range(2):
            pass_on(slot - SETTLE_LAG, side, True)
            pass_on(slot, side, False)
        return carry

    for side in range(2):
        receive(jnp.int32(0), side)
    for load in loads[1:7]:
        load.wait()
    lax.fori_loop(0, items + end_lag + SETTLE_LAG + PASS_LAG, turn, 0)

    def unship(tick):
        sends = me != (my_side if tick else my_start)
        if tick:
            sends = sends & (section == carriers[tick - 1])

        @pl.when(sends)
        def _():
            pltpu.make_async_remote_copy(
                src_ref=x_ref,
                dst_ref=o_ref.at[0],
                send_sem=ship_send.at[tick],
                recv_sem=final_recv.at[0],
                device_id={"section": section, "tensor": me},
                device_id_type=MESH,
            ).wait_send()

    def collect(tick):
        pltpu.make_async_remote_copy(
            src_ref=x_ref,
            dst_ref=o_ref.at[tick],
            send_sem=ship_send.at[0],
            recv_sem=final_recv.at[tick],
            device_id={"section": section, "tensor": me},
            device_id_type=MESH,
        ).wait_recv()

    unship(0)
    collect(TICKS - 1)

    @pl.when(carries)
    def _():
        for tick in range(1, TICKS):
            unship(tick)

    @pl.when(section == 0)
    def _():
        for tick in range(TICKS - 1):
            collect(tick)


def write_kernel(source, target, sem):
    copies = [
        pltpu.make_async_copy(source.at[tick], target.at[tick], sem.at[tick])
        for tick in range(TICKS)
    ]
    for copy in copies:
        copy.start()
    for copy in copies:
        copy.wait()


def write_out(result):
    return pl.pallas_call(
        write_kernel,
        out_shape=jax.ShapeDtypeStruct(result.shape, result.dtype),
        in_specs=[pl.BlockSpec(memory_space=pltpu.VMEM)],
        out_specs=pl.BlockSpec(memory_space=pl.ANY),
        scratch_shapes=[pltpu.SemaphoreType.DMA((TICKS,))],
        compiler_params=pltpu.CompilerParams(vmem_limit_bytes=VMEM_BYTES // 8),
    )(result)


def relay_call(n, sections, pieces, hop_slots, args):
    x, w_in, in_bias, w_out, out_bias, gain, shift, patches, plan = args
    tokens, width = x.shape
    rows = tokens // pieces
    chunks = n // 2 * pieces
    items = TICKS * chunks
    micro = patches.shape[0]
    bf16 = jnp.bfloat16
    vmem = pl.BlockSpec(memory_space=pltpu.VMEM)
    every = (2, items, rows, width)
    dma = pltpu.SemaphoreType.DMA
    out = pl.pallas_call(
        functools.partial(relay_kernel, n, sections, hop_slots),
        out_shape=pltpu.VMEM((TICKS, pieces, rows, width), bf16),
        in_specs=[pl.BlockSpec(memory_space=pl.ANY)] * 9,
        out_specs=vmem,
        scratch_shapes=[
            pltpu.VMEM((pieces, rows, width), bf16),
            pltpu.VMEM(w_in.shape, bf16),
            pltpu.VMEM((1, w_in.shape[0]), bf16),
            pltpu.VMEM(w_out.shape, bf16),
            pltpu.VMEM((1, width), jnp.float32),
            pltpu.VMEM((1, width), jnp.float32),
            pltpu.VMEM((1, width), jnp.float32),
            pltpu.VMEM((micro, pieces, rows, width), bf16),
            pltpu.SMEM(plan.shape, jnp.int32),
            dma((9,)),
            pltpu.VMEM(every, bf16),
            pltpu.VMEM((2,) + every, bf16),
            pltpu.VMEM(every, bf16),
            pltpu.VMEM((TICKS - 1, pieces, rows, width), bf16),
            pltpu.VMEM((TICKS - 1, pieces, rows, width), bf16),
            pltpu.VMEM((2 * rows, width), jnp.float32),
            dma((2, 2, SEND_RING)),
            dma((2, chunks)),
            dma((items - chunks,)),
            dma((2, SEND_RING)),
            dma((2, 2, chunks)),
            dma((TICKS,)),
            dma((pieces,)),
            dma((TICKS - 1, pieces)),
            dma((TICKS,)),
        ],
        compiler_params=pltpu.CompilerParams(
            collective_id=0, has_side_effects=True, vmem_limit_bytes=VMEM_BYTES
        ),
    )(
        x.reshape(pieces, rows, width),
        w_in,
        in_bias.reshape(1, -1),
        w_out,
        out_bias.reshape(1, -1),
        gain.reshape(1, -1),
        shift.reshape(1, -1),
        patches.reshape(micro, pieces, rows, width),
        plan,
    )
    return write_out(out).reshape(1, TICKS, tokens, width)


def passed_along(value, axis, steps):
    count = lax.axis_size(axis)
    pairs = [(source, (source + steps) % count) for source in range(count)]
    return lax.ppermute(value, axis, pairs)


def gathered_weights(args):
    current, w_in, in_bias, w_out, bias_row, gain_row, shift_row, patches, plan = args
    section_index = lax.axis_index("section")
    full_in, full_bias, full_out = (
        lax.all_gather(value, "tensor", axis=0, tiled=True) for value in (w_in, in_bias, w_out)
    )
    records = []
    for tick_index in range(TICKS):
        widened = current.astype(jnp.float32)
        normed = normalize(widened, gain_row, shift_row)
        preact = lax.dot_general(
            normed, full_in, (((1,), (1,)), ((), ())), preferred_element_type=jnp.float32
        )
        hidden = activate(preact + full_bias.astype(jnp.float32)).astype(jnp.bfloat16)
        produced = (
            widened + jnp.dot(hidden, full_out, preferred_element_type=jnp.float32) + bias_row
        ).astype(jnp.bfloat16)
        arrived = passed_along(produced, "section", 1)
        records.append(arrived)
        if tick_index + 1 < TICKS:
            selected = lax.dynamic_index_in_dim(patches, plan[tick_index], 0, keepdims=False)
            current = jnp.where(section_index == 0, selected, arrived)
    return jnp.stack(records, axis=0)[None]


def shards(n, sections, *blocks):
    args = tuple(block[0] for block in blocks[:7]) + blocks[7:]
    tokens, width = args[0].shape
    room = 2 * width * (
        tokens * (TICKS * (5 * n + 2) + 1 + args[7].shape[0]) + 2 * args[1].shape[0]
    )
    if tokens % (PIECES * 16) or n % 2 or sections < 2 or room > VMEM_BYTES * 3 // 4:
        return gathered_weights(args)
    return relay_call(n, sections, PIECES, HOP_SLOTS, args)


def solution(mesh):
    placed = (
        P("section", "tensor", None),
        P("section", "tensor", None),
        P("section", "tensor"),
        P("section", "tensor", None),
        P("section", None),
        P("section", None),
        P("section", None),
        P(None, "tensor", None),
        P(),
    )
    return jax.shard_map(
        functools.partial(shards, mesh.shape["tensor"], mesh.shape["section"]),
        mesh=mesh,
        in_specs=placed,
        out_specs=P("section", None, "tensor", None),
        check_vma=False,
    )
```
